256 devices in a mesh: seq: 128 (over z, x_hi, y, core), ch: 2 (over x_lo).
Axes of the slice: x: 4 (x_hi: 2, x_lo: 2; x = x_hi * 2 + x_lo), y: 4, z: 8, core: 2. Of those that a mesh axis runs over, the one named last changes fastest.
Arguments:
- query_gate: bfloat16 [2, 16384, 2048], P('ch', 'seq'), may hold values from -6 to 6
- key_input: bfloat16 [2, 16384, 2048], P('ch', 'seq'), may hold values from -6 to 6
- value_input: bfloat16 [2, 16384, 2048], P('ch', 'seq'), may hold values from -6 to 6
- grad_output: bfloat16 [2, 16384, 2048], P('ch', 'seq'), may hold values from -6 to 6
- filter_raw: bfloat16 [16384, 2048], P('seq'), may hold values from -6 to 6
- skip_gain: float32 [2048], replicated, may hold values from 0.5 to 1.5
Outputs:
- grad_query: bfloat16 [2, 16384, 2048], P('ch', 'seq')
- grad_key: bfloat16 [2, 16384, 2048], P('ch', 'seq')
- grad_value: bfloat16 [2, 16384, 2048], P('ch', 'seq')
- grad_filter: float32 [16384, 2048], P('seq', 'ch')
The draws below stay inside these ranges and needn't reach their ends.
All inputs are finite; a program needn't handle non-finite values.
Results may differ from the reference program's by a relative error of at most 0.001.
Values sent between devices are 32-bit elements; how exact they have to be, the bound alone decides.
A program may use at most 128 MiB of HBM per device.

```python
import jax
import jax.numpy as jnp
from jax import lax

CHANNELS = 2048
SEQ_LEN = 16384
BATCH = 2


def block_levels(stream_key, extent, cuts, smallest, high):
    def one(axis_at, parts):
        draws = jax.random.uniform(jax.random.fold_in(jax.random.fold_in(stream_key, 6), axis_at), (parts,), jnp.float32, smallest / len(cuts), high / len(cuts))
        return jnp.repeat(jnp.exp(draws), extent[axis_at] // parts).reshape((-1,) + (1,) * (len(extent) - axis_at - 1))

    loudness = one(*cuts[0])
    for cut in cuts[1:]:
        loudness = loudness * one(*cut)
    return loudness


def gaussian(rng, dims, deviation, most, cuts=(), dtype=jnp.bfloat16):
    drawn = deviation * jax.random.normal(rng, dims, jnp.float32)
    if cuts:
        drawn = drawn * block_levels(rng, dims, cuts, -0.22, 0.18)
    return jnp.clip(drawn, -most, most).astype(dtype)


def setup_inputs(seed: int = 0) -> dict:
    key_list = jax.random.split(jax.random.key(seed), 7)
    return {
        "query_gate": gaussian(key_list[0], (BATCH, SEQ_LEN, CHANNELS), 1.0, 6.0, ((0, 2), (1, 128))),
        "key_input": gaussian(key_list[1], (BATCH, SEQ_LEN, CHANNELS), 1.0, 6.0, ((0, 2), (1, 128))),
        "value_input": gaussian(key_list[2], (BATCH, SEQ_LEN, CHANNELS), 1.0, 6.0, ((0, 2), (1, 128))),
        "grad_output": gaussian(key_list[3], (BATCH, SEQ_LEN, CHANNELS), 1.0, 6.0, ((0, 2), (1, 128))),
        "filter_raw": gaussian(key_list[4], (SEQ_LEN, CHANNELS), 1.0, 6.0, ((0, 128),)),
        "skip_gain": jnp.clip(jax.random.uniform(key_list[5], (CHANNELS,), jnp.float32, 0.5, 1.5), 0.5, 1.5),
    }


def block_grads(pieces):
    query_gate, key_input, value_input, grad_output, filter_raw, skip_gain = pieces
    length = 2 * SEQ_LEN
    filter_taps = filter_raw.astype(jnp.float32) * (SEQ_LEN ** -0.5)
    filter_spec = jnp.fft.rfft(filter_taps, n=length, axis=0)
    grads_query = []
    grads_key = []
    grads_value = []
    corr_total = jnp.zeros(filter_taps.shape, jnp.float32)
    for seq_index in range(BATCH):
        key_f = key_input[seq_index].astype(jnp.float32)
        value_f = value_input[seq_index].astype(jnp.float32)
        out_f = grad_output[seq_index].astype(jnp.float32)
        query_f = query_gate[seq_index].astype(jnp.float32)
        mixed_signal = key_f * value_f
        gated_grad = out_f * query_f
        mixed_spec = jnp.fft.rfft(mixed_signal, n=length, axis=0)
        gated_spec = jnp.fft.rfft(gated_grad, n=length, axis=0)
        conv_out = jnp.fft.irfft(mixed_spec * filter_spec, n=length, axis=0)[:SEQ_LEN] + skip_gain * mixed_signal
        back_grad = jnp.fft.irfft(jnp.conj(filter_spec) * gated_spec, n=length, axis=0)[:SEQ_LEN] + skip_gain * gated_grad
        corr_grad = jnp.fft.irfft(jnp.conj(mixed_spec) * gated_spec, n=length, axis=0)[:SEQ_LEN]
        grads_query.append((out_f * conv_out).astype(jnp.bfloat16))
        grads_key.append((back_grad * value_f).astype(jnp.bfloat16))
        grads_value.append((back_grad * key_f).astype(jnp.bfloat16))
        corr_total = corr_total + corr_grad
    return (jnp.stack(grads_query), jnp.stack(grads_key), jnp.stack(grads_value),
            corr_total * (SEQ_LEN ** -0.5))


def reference(query_gate, key_input, value_input, grad_output, filter_raw, skip_gain):
    channel_width = CHANNELS
    block_size = 256 if channel_width % 256 == 0 else channel_width
    groups = channel_width // block_size

    def split_channels(tensor_in):
        reshaped = tensor_in.reshape(tensor_in.shape[:-1] + (groups, block_size))
        return jnp.moveaxis(reshaped, -2, 0)

    def join_channels(tensor_in):
        reshaped = jnp.moveaxis(tensor_in, 0, -2)
        return reshaped.reshape(reshaped.shape[:-2] + (channel_width,))

    stacked = (split_channels(query_gate), split_channels(key_input), split_channels(value_input),
               split_channels(grad_output), split_channels(filter_raw), split_channels(skip_gain))
    results = lax.map(block_grads, stacked)
    return (join_channels(results[0]), join_channels(results[1]), join_channels(results[2]),
            join_channels(results[3]))
```

```python
import functools
import math

import jax
import jax.numpy as jnp
import numpy as np
from jax import lax
from jax.experimental import pallas as pl
from jax.experimental.pallas import tpu as pltpu
from jax.sharding import PartitionSpec as P

BLOCK = 128
FULL = 2 * BLOCK * BLOCK
F32 = jnp.float32
BF16 = jnp.bfloat16


def split_table(table):
    high = jnp.asarray(table, F32).astype(BF16)
    low = (jnp.asarray(table, F32) - high.astype(F32)).astype(BF16)
    return (high, low)


def tables():
    idx = np.arange(BLOCK)
    turn_one = 2.0 * math.pi / (2 * BLOCK) * ((idx[:, None] + 0.5) * idx[None, :])
    first = np.concatenate([np.cos(turn_one), -np.sin(turn_one)], axis=0)
    turn_two = 2.0 * math.pi / BLOCK * (idx[:, None] * idx[None, :] % BLOCK)
    cos_two, sin_two = np.cos(turn_two), np.sin(turn_two)
    second = np.block([[cos_two, -sin_two], [sin_two, cos_two]])
    second_inv = np.block([[cos_two, sin_two], [-sin_two, cos_two]])
    turn_mid = 2.0 * math.pi / FULL * ((idx[:, None] + 0.5) * idx[None, :])
    out = []
    for table in (first, second, second_inv, first.T):
        out.extend(split_table(table.astype(np.float32)))
    out.append(jnp.asarray(np.cos(turn_mid), F32))
    out.append(jnp.asarray(np.sin(turn_mid), F32))
    return tuple(out)


def halves(x):
    high = x.astype(BF16)
    return (high, (x - high.astype(F32)).astype(BF16))


def dot(a, b):
    return jnp.dot(a, b, preferred_element_type=F32)


def dot_left(high, low, x):
    x_high, x_low = halves(x)
    return dot(high, x_high) + dot(low, x_high) + dot(high, x_low)


def dot_right(x, high, low):
    x_high, x_low = halves(x)
    return dot(x_high, high) + dot(x_high, low) + dot(x_low, high)


def to_spectrum(parts, tab):
    f_high, f_low, s_high, s_low = tab[0][...], tab[1][...], tab[2][...], tab[3][...]
    cos_mid, sin_mid = tab[8][...], tab[9][...]
    lines = dot_left(f_high, f_low, jnp.concatenate(parts, axis=1))
    rows = []
    for i in range(len(parts)):
        re = lines[:BLOCK, i * BLOCK : (i + 1) * BLOCK]
        im = lines[BLOCK:, i * BLOCK : (i + 1) * BLOCK]
        rows.append(
            jnp.concatenate([re * cos_mid + im * sin_mid, im * cos_mid - re * sin_mid], axis=1)
        )
    spec = dot_right(jnp.concatenate(rows, axis=0), s_high, s_low)
    return [
        (spec[i * BLOCK : (i + 1) * BLOCK, :BLOCK], spec[i * BLOCK : (i + 1) * BLOCK, BLOCK:])
        for i in range(len(parts))
    ]


def from_spectrum(specs, tab):
    i_high, i_low, t_high, t_low = tab[4][...], tab[5][...], tab[6][...], tab[7][...]
    cos_mid, sin_mid = tab[8][...], tab[9][...]
    rows = jnp.concatenate([jnp.concatenate([re, im], axis=1) for re, im in specs], axis=0)
    mid = dot_right(rows, i_high, i_low)
    cols = []
    for i in range(len(specs)):
        re = mid[i * BLOCK : (i + 1) * BLOCK, :BLOCK]
        im = mid[i * BLOCK : (i + 1) * BLOCK, BLOCK:]
        cols.append(
            jnp.concatenate([re * cos_mid - im * sin_mid, im * cos_mid + re * sin_mid], axis=0)
        )
    lines = dot_left(t_high, t_low, jnp.concatenate(cols, axis=1))
    return [lines[:, i * BLOCK : (i + 1) * BLOCK] for i in range(len(specs))]


SCALE = 1.0 / (BLOCK * (FULL // 2))


def channel_rows(part, channel):
    return pl.ds(part * BLOCK * 8 + channel, BLOCK, stride=8)


def conv_kernel(*refs):
    tab, (mixed_ref, taps_ref, conv_ref, mspec_ref, tspec_ref) = refs[:10], refs[10:]

    def body(c, carry):
        parts = [mixed_ref[channel_rows(b, c), :] for b in range(2)]
        parts.append(taps_ref[channel_rows(0, c), :])
        mixed_a, mixed_b, taps = to_spectrum(parts, tab)
        prods = []
        for b, (re, im) in enumerate((mixed_a, mixed_b)):
            mspec_ref[c, b, 0] = re
            mspec_ref[c, b, 1] = im
            prods.append((re * taps[0] - im * taps[1], re * taps[1] + im * taps[0]))
        tspec_ref[c, 0] = taps[0]
        tspec_ref[c, 1] = taps[1]
        lines = from_spectrum(prods, tab)
        for b in range(2):
            conv_ref[channel_rows(b, c), :] = lines[b] * SCALE
        return carry

    lax.fori_loop(0, 8, body, 0)


def back_kernel(*refs):
    tab, (gated_ref, mspec_ref, tspec_ref, back_ref, corr_ref) = refs[:10], refs[10:]

    def body(c, carry):
        gated = to_spectrum([gated_ref[channel_rows(b, c), :] for b in range(2)], tab)
        t_re, t_im = tspec_ref[c, 0], tspec_ref[c, 1]
        prods = []
        corr_re = corr_im = None
        for b, (re, im) in enumerate(gated):
            m_re, m_im = mspec_ref[c, b, 0], mspec_ref[c, b, 1]
            prods.append((t_re * re + t_im * im, t_re * im - t_im * re))
            term_re = m_re * re + m_im * im
            term_im = m_re * im - m_im * re
            corr_re = term_re if corr_re is None else corr_re + term_re
            corr_im = term_im if corr_im is None else corr_im + term_im
        prods.append((corr_re, corr_im))
        lines = from_spectrum(prods, tab)
        for b in range(2):
            back_ref[channel_rows(b, c), :] = lines[b] * SCALE
        corr_ref[channel_rows(0, c), :] = lines[2] * SCALE
        return carry

    lax.fori_loop(0, 8, body, 0)


def call(kernel, out_shapes, operands, name):
    vmem = pl.BlockSpec(memory_space=pltpu.VMEM)
    return pl.pallas_call(
        kernel,
        out_shape=[jax.ShapeDtypeStruct(s, F32) for s in out_shapes],
        in_specs=[vmem] * len(operands),
        out_specs=[vmem] * len(out_shapes),
        cost_estimate=pl.CostEstimate(
            flops=6_000_000_000, bytes_accessed=6_000_000, transcendentals=0
        ),
        compiler_params=pltpu.CompilerParams(vmem_limit_bytes=40 * 1024 * 1024),
        name=name,
    )(*operands)


def exchange(rows, axes):
    return lax.all_to_all(rows.reshape(-1, 8, BLOCK), axes, 0, 0, tiled=True).reshape(-1, BLOCK)


def shards(query_gate, key_input, value_input, grad_output, filter_raw, skip_gain):
    tab = tables()
    key_f = key_input[0].astype(F32)
    value_f = value_input[0].astype(F32)
    out_f = grad_output[0].astype(F32)
    mixed = key_f * value_f
    gated = out_f * query_gate[0].astype(F32)
    half = filter_raw.shape[1] // 2
    taps = lax.dynamic_slice_in_dim(filter_raw, lax.axis_index("ch") * half, half, 1)
    both = ("ch", "seq")
    mixed_in = exchange(mixed.T, both)
    taps_in = exchange(taps.T.astype(F32), "seq")
    gated_in = exchange(gated.T, both)
    conv, mspec, tspec = call(
        conv_kernel,
        [(2048, BLOCK), (8, 2, 2, BLOCK, BLOCK), (8, 2, BLOCK, BLOCK)],
        (*tab, mixed_in, taps_in),
        "conv_part",
    )
    back, corr = call(
        back_kernel,
        [(2048, BLOCK), (1024, BLOCK)],
        (*tab, gated_in, mspec, tspec),
        "back_part",
    )
    conv_time = exchange(conv, both).T
    back_time = exchange(back, both).T
    grad_filter = exchange(corr, "seq").T
    conv_full = conv_time + skip_gain * mixed
    back_full = back_time + skip_gain * gated
    grad_query = (out_f * conv_full).astype(BF16)[None]
    grad_key = (back_full * value_f).astype(BF16)[None]
    grad_value = (back_full * key_f).astype(BF16)[None]
    return (grad_query, grad_key, grad_value, grad_filter)


def solution(mesh):
    in_specs = (
        P("ch", "seq", None),
        P("ch", "seq", None),
        P("ch", "seq", None),
        P("ch", "seq", None),
        P("seq", None),
        P(),
    )
    out_specs = (P("ch", "seq", None), P("ch", "seq", None), P("ch", "seq", None), P("seq", "ch"))
    return jax.shard_map(shards, mesh=mesh, in_specs=in_specs, out_specs=out_specs, check_vma=False)
```

```python
import math

import jax
import jax.numpy as jnp
import numpy as np
from jax import lax
from jax.experimental import pallas as pl
from jax.experimental.pallas import tpu as pltpu
from jax.sharding import PartitionSpec as P

BLOCK = 128
FULL = 2 * BLOCK * BLOCK
F32 = jnp.float32
BF16 = jnp.bfloat16


def split_table(table):
    high = jnp.asarray(table, F32).astype(BF16)
    low = (jnp.asarray(table, F32) - high.astype(F32)).astype(BF16)
    return (high, low)


def tables():
    idx = np.arange(BLOCK)
    turn_one = 2.0 * math.pi / (2 * BLOCK) * ((idx[:, None] + 0.5) * idx[None, :])
    first = np.concatenate([np.cos(turn_one), -np.sin(turn_one)], axis=0)
    turn_two = 2.0 * math.pi / BLOCK * (idx[:, None] * idx[None, :] % BLOCK)
    cos_two, sin_two = np.cos(turn_two), np.sin(turn_two)
    second = np.block([[cos_two, -sin_two], [sin_two, cos_two]])
    second_inv = np.block([[cos_two, sin_two], [-sin_two, cos_two]])
    turn_mid = 2.0 * math.pi / FULL * ((idx[:, None] + 0.5) * idx[None, :])
    f_high, f_low = split_table(first.astype(np.float32))
    rows = [jnp.concatenate([f_high, f_low], axis=1)]
    for table in (second, second_inv, first.T):
        rows.extend(split_table(table.astype(np.float32)))
    mid = np.concatenate([np.cos(turn_mid), np.sin(turn_mid)], axis=0)
    return (jnp.concatenate(rows, axis=0), jnp.asarray(mid, F32))


def halves(x):
    high = x.astype(BF16)
    return (high, (x - high.astype(F32)).astype(BF16))


def dot(a, b):
    return jnp.dot(a, b, preferred_element_type=F32)


def dot_left(high, low, x):
    x_high, x_low = halves(x)
    return dot(high, x_high) + dot(low, x_high) + dot(high, x_low)


def dot_right(x, high, low):
    x_high, x_low = halves(x)
    return dot(x_high, high) + dot(x_high, low) + dot(x_low, high)


def to_spectrum(parts, tab, mid):
    cos_mid, sin_mid = mid[:BLOCK], mid[BLOCK:]
    lines = dot_left(tab[:256, :BLOCK], tab[:256, BLOCK:], jnp.concatenate(parts, axis=1))
    rows = []
    for i in range(len(parts)):
        re = lines[:BLOCK, i * BLOCK : (i + 1) * BLOCK]
        im = lines[BLOCK:, i * BLOCK : (i + 1) * BLOCK]
        rows.append(
            jnp.concatenate([re * cos_mid + im * sin_mid, im * cos_mid - re * sin_mid], axis=1)
        )
    spec = dot_right(jnp.concatenate(rows, axis=0), tab[256:512], tab[512:768])
    return [
        (spec[i * BLOCK : (i + 1) * BLOCK, :BLOCK], spec[i * BLOCK : (i + 1) * BLOCK, BLOCK:])
        for i in range(len(parts))
    ]


def from_spectrum(specs, tab, mid):
    cos_mid, sin_mid = mid[:BLOCK], mid[BLOCK:]
    rows = jnp.concatenate([jnp.concatenate([re, im], axis=1) for re, im in specs], axis=0)
    grid = dot_right(rows, tab[768:1024], tab[1024:1280])
    cols = []
    for i in range(len(specs)):
        re = grid[i * BLOCK : (i + 1) * BLOCK, :BLOCK]
        im = grid[i * BLOCK : (i + 1) * BLOCK, BLOCK:]
        cols.append(
            jnp.concatenate([re * cos_mid - im * sin_mid, im * cos_mid + re * sin_mid], axis=0)
        )
    lines = dot_left(tab[1280:1408], tab[1408:1536], jnp.concatenate(cols, axis=1))
    return [lines[:, i * BLOCK : (i + 1) * BLOCK] for i in range(len(specs))]


SCALE = 1.0 / (BLOCK * (FULL // 2))
OWNED = 8
WIDTH = 2048
HALF = WIDTH // 2
MESH = pl.DeviceIdType.MESH


def channel_rows(part, channel):
    return pl.ds(part * BLOCK * OWNED + channel, BLOCK, stride=OWNED)


def tile(index):
    return pl.ds(pl.multiple_of(index * OWNED, OWNED), OWNED)


def peer(step, seq, ch):
    turn = step % 8
    near = (turn + 1) // 2
    shift = (turn % 2) * near + (1 - turn % 2) * (8 - near)
    z = (seq // 16 + shift) % 8
    rest = ((seq % 16) * 2 + ch + step // 8) % 32
    return (z * 16 + rest // 2, rest % 2)


def peer_same(step, seq):
    turn = step % 8
    near = (turn + 1) // 2
    shift = (turn % 2) * near + (1 - turn % 2) * (8 - near)
    z = (seq // 16 + shift) % 8
    return z * 16 + (seq % 16 + step // 8) % 16


def send_all(source, target, send, recv):
    seq, ch = lax.axis_index("seq"), lax.axis_index("ch")
    me = ch * BLOCK + seq

    def body(step, carry):
        to_seq, to_ch = peer(step, seq, ch)
        pltpu.make_async_remote_copy(
            src_ref=source.at[tile(to_ch * BLOCK + to_seq)],
            dst_ref=target.at[tile(me)],
            send_sem=send,
            recv_sem=recv,
            device_id=(to_seq, to_ch),
            device_id_type=MESH,
        ).start()
        return carry

    lax.fori_loop(1, 2 * BLOCK, body, 0)
    target[tile(me), :] = source[tile(me), :]


def send_same(source, target, send, recv):
    seq, ch = lax.axis_index("seq"), lax.axis_index("ch")

    def body(step, carry):
        to_seq = peer_same(step, seq)
        pltpu.make_async_remote_copy(
            src_ref=source.at[tile(to_seq)],
            dst_ref=target.at[tile(seq)],
            send_sem=send,
            recv_sem=recv,
            device_id=(to_seq, ch),
            device_id_type=MESH,
        ).start()
        return carry

    lax.fori_loop(1, BLOCK, body, 0)
    target[tile(seq), :] = source[tile(seq), :]


def wait_rows(ref, rows, sem):
    part = ref.at[pl.ds(0, rows)]
    pltpu.make_async_copy(part, part, sem).wait()


ALL_ROWS = WIDTH - OWNED
SAME_ROWS = HALF - OWNED


def kernel(
    query_hbm,
    key_hbm,
    value_hbm,
    out_hbm,
    filter_hbm,
    gain_ref,
    tab_hbm,
    mid_hbm,
    grad_query,
    grad_key,
    grad_value,
    grad_filter,
    query,
    key,
    value,
    out,
    taps,
    tab_ref,
    mid_ref,
    mixed_t,
    gated_t,
    taps_t,
    mixed_in,
    gated_in,
    taps_in,
    conv,
    back,
    corr,
    conv_in,
    back_in,
    corr_in,
    mspec,
    tspec,
    load,
    send,
    recv,
):
    seq, ch = lax.axis_index("seq"), lax.axis_index("ch")
    barrier = pltpu.get_barrier_semaphore()

    loads = [
        pltpu.make_async_copy(key_hbm.at[0], key, load.at[0]),
        pltpu.make_async_copy(value_hbm.at[0], value, load.at[1]),
        pltpu.make_async_copy(
            filter_hbm.at[:, pl.ds(pl.multiple_of(ch * HALF, HALF), HALF)], taps, load.at[2]
        ),
        pltpu.make_async_copy(out_hbm.at[0], out, load.at[3]),
        pltpu.make_async_copy(query_hbm.at[0], query, load.at[4]),
        pltpu.make_async_copy(tab_hbm, tab_ref, load.at[5]),
        pltpu.make_async_copy(mid_hbm, mid_ref, load.at[6]),
    ]
    for copy in loads:
        copy.start()

    def greet(step, carry):
        to_seq, to_ch = peer(step, seq, ch)
        pl.semaphore_signal(barrier, inc=1, device_id=(to_seq, to_ch), device_id_type=MESH)
        return carry

    lax.fori_loop(1, 2 * BLOCK, greet, 0)

    def flip_product(left, right, target):
        def body(j, carry):
            cols = pl.ds(pl.multiple_of(j * BLOCK, BLOCK), BLOCK)
            target[cols, :] = (left[:, cols].astype(F32) * right[:, cols].astype(F32)).T
            return carry

        lax.fori_loop(0, WIDTH // BLOCK, body, 0)

    loads[0].wait()
    loads[1].wait()
    flip_product(key, value, mixed_t)
    loads[2].wait()

    def flip_taps(j, carry):
        cols = pl.ds(pl.multiple_of(j * BLOCK, BLOCK), BLOCK)
        taps_t[cols, :] = taps[:, cols].astype(F32).T
        return carry

    lax.fori_loop(0, HALF // BLOCK, flip_taps, 0)
    pl.semaphore_wait(barrier, 2 * BLOCK - 1)
    send_all(mixed_t, mixed_in, send.at[0], recv.at[0])
    send_same(taps_t, taps_in, send.at[1], recv.at[1])
    loads[3].wait()
    loads[4].wait()
    flip_product(out, query, gated_t)
    send_all(gated_t, gated_in, send.at[2], recv.at[2])
    loads[5].wait()
    loads[6].wait()
    wait_rows(mixed_in, ALL_ROWS, recv.at[0])
    wait_rows(taps_in, SAME_ROWS, recv.at[1])

    def conv_body(c, carry):
        tab, mid = tab_ref[...], mid_ref[...]
        parts = [mixed_in[channel_rows(b, c), :] for b in range(2)]
        parts.append(taps_in[channel_rows(0, c), :])
        mixed_a, mixed_b, taps_spec = to_spectrum(parts, tab, mid)
        t_re, t_im = taps_spec
        prods = []
        for b, (re, im) in enumerate((mixed_a, mixed_b)):
            mspec[c, b, 0] = re
            mspec[c, b, 1] = im
            prods.append((re * t_re - im * t_im, re * t_im + im * t_re))
        tspec[c, 0] = t_re
        tspec[c, 1] = t_im
        lines = from_spectrum(prods, tab, mid)
        for b in range(2):
            conv[channel_rows(b, c), :] = lines[b] * SCALE
        return carry

    lax.fori_loop(0, OWNED, conv_body, 0)
    send_all(conv, conv_in, send.at[3], recv.at[3])
    wait_rows(gated_in, ALL_ROWS, recv.at[2])

    def back_body(c, carry):
        tab, mid = tab_ref[...], mid_ref[...]
        gated = to_spectrum([gated_in[channel_rows(b, c), :] for b in range(2)], tab, mid)
        t_re, t_im = tspec[c, 0], tspec[c, 1]
        prods = []
        terms = []
        for b, (re, im) in enumerate(gated):
            m_re, m_im = mspec[c, b, 0], mspec[c, b, 1]
            prods.append((t_re * re + t_im * im, t_re * im - t_im * re))
            terms.append((m_re * re + m_im * im, m_re * im - m_im * re))
        prods.append((terms[0][0] + terms[1][0], terms[0][1] + terms[1][1]))
        lines = from_spectrum(prods, tab, mid)
        for b in range(2):
            back[channel_rows(b, c), :] = lines[b] * SCALE
        corr[channel_rows(0, c), :] = lines[2] * SCALE
        return carry

    lax.fori_loop(0, OWNED, back_body, 0)
    send_all(back, back_in, send.at[4], recv.at[4])
    send_same(corr, corr_in, send.at[5], recv.at[5])

    wait_rows(conv_in, ALL_ROWS, recv.at[3])

    def query_body(j, carry):
        cols = pl.ds(pl.multiple_of(j * BLOCK, BLOCK), BLOCK)
        mixed = key[:, cols].astype(F32) * value[:, cols].astype(F32)
        full = conv_in[cols, :].T + gain_ref[:, cols] * mixed
        grad_query[0, :, cols] = (out[:, cols].astype(F32) * full).astype(BF16)
        return carry

    lax.fori_loop(0, WIDTH // BLOCK, query_body, 0)
    wait_rows(back_in, ALL_ROWS, recv.at[4])

    def back_out(j, carry):
        cols = pl.ds(pl.multiple_of(j * BLOCK, BLOCK), BLOCK)
        gated = out[:, cols].astype(F32) * query[:, cols].astype(F32)
        full = back_in[cols, :].T + gain_ref[:, cols] * gated
        grad_key[0, :, cols] = (full * value[:, cols].astype(F32)).astype(BF16)
        grad_value[0, :, cols] = (full * key[:, cols].astype(F32)).astype(BF16)
        return carry

    lax.fori_loop(0, WIDTH // BLOCK, back_out, 0)
    wait_rows(corr_in, SAME_ROWS, recv.at[5])

    def filter_out(j, carry):
        cols = pl.ds(pl.multiple_of(j * BLOCK, BLOCK), BLOCK)
        grad_filter[:, cols] = corr_in[cols, :].T
        return carry

    lax.fori_loop(0, HALF // BLOCK, filter_out, 0)
    wait_rows(mixed_t, ALL_ROWS, send.at[0])
    wait_rows(taps_t, SAME_ROWS, send.at[1])
    wait_rows(gated_t, ALL_ROWS, send.at[2])
    wait_rows(conv, ALL_ROWS, send.at[3])
    wait_rows(back, ALL_ROWS, send.at[4])
    wait_rows(corr, SAME_ROWS, send.at[5])


def shards(query_gate, key_input, value_input, grad_output, filter_raw, skip_gain):
    tab, mid = tables()
    anywhere = pl.BlockSpec(memory_space=pl.ANY)
    vmem = pl.BlockSpec(memory_space=pltpu.VMEM)
    signal = jax.ShapeDtypeStruct((1, BLOCK, WIDTH), BF16)
    narrow = pltpu.VMEM((BLOCK, WIDTH), BF16)
    tall = pltpu.VMEM((WIDTH, BLOCK), F32)
    short = pltpu.VMEM((HALF, BLOCK), F32)
    return tuple(
        pl.pallas_call(
            kernel,
            out_shape=[signal, signal, signal, jax.ShapeDtypeStruct((BLOCK, HALF), F32)],
            in_specs=[anywhere] * 5 + [vmem] + [anywhere] * 2,
            out_specs=[vmem] * 4,
            scratch_shapes=[narrow] * 4
            + [
                pltpu.VMEM((BLOCK, HALF), BF16),
                pltpu.VMEM(tab.shape, BF16),
                pltpu.VMEM(mid.shape, F32),
            ]
            + [tall, tall, short] * 4
            + [
                pltpu.VMEM((OWNED, 2, 2, BLOCK, BLOCK), F32),
                pltpu.VMEM((OWNED, 2, BLOCK, BLOCK), F32),
                pltpu.SemaphoreType.DMA((7,)),
                pltpu.SemaphoreType.DMA((6,)),
                pltpu.SemaphoreType.DMA((6,)),
            ],
            compiler_params=pltpu.CompilerParams(
                collective_id=0, has_side_effects=True, vmem_limit_bytes=60 * 1024 * 1024
            ),
            name="hyena_back",
        )(
            query_gate,
            key_input,
            value_input,
            grad_output,
            filter_raw,
            skip_gain.reshape(1, WIDTH),
            tab,
            mid,
        )
    )


def solution(mesh):
    in_specs = (
        P("ch", "seq", None),
        P("ch", "seq", None),
        P("ch", "seq", None),
        P("ch", "seq", None),
        P("seq", None),
        P(),
    )
    out_specs = (P("ch", "seq", None), P("ch", "seq", None), P("ch", "seq", None), P("seq", "ch"))
    return jax.shard_map(shards, mesh=mesh, in_specs=in_specs, out_specs=out_specs, check_vma=False)
```

```python
import math

import jax
import jax.numpy as jnp
import numpy as np
from jax import lax
from jax.experimental import pallas as pl
from jax.experimental.pallas import tpu as pltpu
from jax.sharding import PartitionSpec as P

BLOCK = 128
FULL = 2 * BLOCK * BLOCK
F32 = jnp.float32
BF16 = jnp.bfloat16


def split_table(table):
    high = jnp.asarray(table, F32).astype(BF16)
    low = (jnp.asarray(table, F32) - high.astype(F32)).astype(BF16)
    return (high, low)


def tables():
    idx = np.arange(BLOCK)
    turn_one = 2.0 * math.pi / (2 * BLOCK) * ((idx[:, None] + 0.5) * idx[None, :])
    first = np.concatenate([np.cos(turn_one), -np.sin(turn_one)], axis=0)
    turn_two = 2.0 * math.pi / BLOCK * (idx[:, None] * idx[None, :] % BLOCK)
    cos_two, sin_two = np.cos(turn_two), np.sin(turn_two)
    second = np.block([[cos_two, -sin_two], [sin_two, cos_two]])
    second_inv = np.block([[cos_two, sin_two], [-sin_two, cos_two]])
    turn_mid = 2.0 * math.pi / FULL * ((idx[:, None] + 0.5) * idx[None, :])
    f_high, f_low = split_table(first.astype(np.float32))
    rows = [jnp.concatenate([f_high, f_low], axis=1)]
    for table in (second, second_inv, first.T):
        rows.extend(split_table(table.astype(np.float32)))
    mid = np.concatenate([np.cos(turn_mid), np.sin(turn_mid)], axis=0)
    return (jnp.concatenate(rows, axis=0), jnp.asarray(mid, F32))


def halves(x):
    high = x.astype(BF16)
    return (high, (x - high.astype(F32)).astype(BF16))


def dot(a, b):
    return jnp.dot(a, b, preferred_element_type=F32)


def dot_left(high, low, x):
    x_high, x_low = halves(x)
    return dot(high, x_high) + dot(low, x_high) + dot(high, x_low)


def dot_right(x, high, low):
    x_high, x_low = halves(x)
    return dot(x_high, high) + dot(x_high, low) + dot(x_low, high)


def to_spectrum(parts, tab, mid):
    cos_mid, sin_mid = mid[:BLOCK], mid[BLOCK:]
    lines = dot_left(tab[:256, :BLOCK], tab[:256, BLOCK:], jnp.concatenate(parts, axis=1))
    rows = []
    for i in range(len(parts)):
        re = lines[:BLOCK, i * BLOCK : (i + 1) * BLOCK]
        im = lines[BLOCK:, i * BLOCK : (i + 1) * BLOCK]
        rows.append(
            jnp.concatenate([re * cos_mid + im * sin_mid, im * cos_mid - re * sin_mid], axis=1)
        )
    spec = dot_right(jnp.concatenate(rows, axis=0), tab[256:512], tab[512:768])
    return [
        (spec[i * BLOCK : (i + 1) * BLOCK, :BLOCK], spec[i * BLOCK : (i + 1) * BLOCK, BLOCK:])
        for i in range(len(parts))
    ]


def from_spectrum(specs, tab, mid):
    cos_mid, sin_mid = mid[:BLOCK], mid[BLOCK:]
    rows = jnp.concatenate([jnp.concatenate([re, im], axis=1) for re, im in specs], axis=0)
    grid = dot_right(rows, tab[768:1024], tab[1024:1280])
    cols = []
    for i in range(len(specs)):
        re = grid[i * BLOCK : (i + 1) * BLOCK, :BLOCK]
        im = grid[i * BLOCK : (i + 1) * BLOCK, BLOCK:]
        cols.append(
            jnp.concatenate([re * cos_mid - im * sin_mid, im * cos_mid + re * sin_mid], axis=0)
        )
    lines = dot_left(tab[1280:1408], tab[1408:1536], jnp.concatenate(cols, axis=1))
    return [lines[:, i * BLOCK : (i + 1) * BLOCK] for i in range(len(specs))]


SCALE = 1.0 / (BLOCK * (FULL // 2))
OWNED = 8
WIDTH = 2048
HALF = WIDTH // 2
MESH = pl.DeviceIdType.MESH


def channel_rows(part, channel):
    return pl.ds(part * BLOCK * OWNED + channel, BLOCK, stride=OWNED)


def tile(index):
    return pl.ds(pl.multiple_of(index * OWNED, OWNED), OWNED)


TURNS = (0, 1, 7, 2, 6, 3, 5, 4)
SLAB = BLOCK // 8
FAR_FIRST = ((4, 0), (3, 5), (2, 6), (1, 7))


def for_each_peer(visit, turns=TURNS):
    seq, ch = lax.axis_index("seq"), lax.axis_index("ch")
    z = lax.div(seq, SLAB)
    place = lax.rem(seq, SLAB) * 2 + ch
    bases = [lax.rem(z + turn, 8) * SLAB for turn in turns]

    def at(rest, chosen):
        low, to_ch = lax.div(rest, 2), lax.rem(rest, 2)
        for base in chosen:
            visit(base + low, to_ch)

    def body(step, carry):
        at(lax.rem(place + step, 2 * SLAB), bases)
        return carry

    at(place, [base for base, turn in zip(bases, turns) if turn])
    lax.fori_loop(1, 2 * SLAB, body, 0)


def for_each_same(visit, groups=(TURNS,)):
    seq = lax.axis_index("seq")
    z = lax.div(seq, SLAB)
    place = lax.rem(seq, SLAB)
    for turns in groups:
        bases = [lax.rem(z + turn, 8) * SLAB for turn in turns]

        def body(step, carry, bases=bases):
            low = lax.rem(place + step, SLAB)
            for base in bases:
                visit(base + low)
            return carry

        for base, turn in zip(bases, turns):
            if turn:
                visit(base + place)
        lax.fori_loop(1, SLAB, body, 0)


def send_all(source, target, send, recv):
    seq, ch = lax.axis_index("seq"), lax.axis_index("ch")
    me = ch * BLOCK + seq

    def visit(to_seq, to_ch):
        pltpu.make_async_remote_copy(
            src_ref=source.at[tile(to_ch * BLOCK + to_seq)],
            dst_ref=target.at[tile(me)],
            send_sem=send,
            recv_sem=recv,
            device_id=(to_seq, to_ch),
            device_id_type=MESH,
        ).start()

    for_each_peer(visit)
    target[tile(me), :] = source[tile(me), :]


def send_same(source, target, send, recv, groups=(TURNS,)):
    seq, ch = lax.axis_index("seq"), lax.axis_index("ch")

    def visit(to_seq):
        pltpu.make_async_remote_copy(
            src_ref=source.at[tile(to_seq)],
            dst_ref=target.at[tile(seq)],
            send_sem=send,
            recv_sem=recv,
            device_id=(to_seq, ch),
            device_id_type=MESH,
        ).start()

    for_each_same(visit, groups)
    target[tile(seq), :] = source[tile(seq), :]


def wait_rows(ref, rows, sem):
    part = ref.at[pl.ds(0, rows)]
    pltpu.make_async_copy(part, part, sem).wait()


ALL_ROWS = WIDTH - OWNED
SAME_ROWS = HALF - OWNED


def kernel(
    query_hbm,
    key_hbm,
    value_hbm,
    out_hbm,
    filter_hbm,
    gain_hbm,
    tab_hbm,
    mid_hbm,
    grad_query,
    grad_key,
    grad_value,
    corr_in,
    query,
    key,
    value,
    out,
    taps,
    tab_ref,
    mid_ref,
    gain_ref,
    mixed_t,
    gated_t,
    taps_t,
    mixed_in,
    gated_in,
    taps_in,
    conv,
    back,
    corr,
    conv_in,
    back_in,
    mspec,
    tspec,
    load,
    send,
    recv,
):
    seq, ch = lax.axis_index("seq"), lax.axis_index("ch")
    barrier = pltpu.get_barrier_semaphore()

    loads = [
        pltpu.make_async_copy(key_hbm.at[0], key, load.at[0]),
        pltpu.make_async_copy(value_hbm.at[0], value, load.at[1]),
        pltpu.make_async_copy(
            filter_hbm.at[:, pl.ds(pl.multiple_of(ch * HALF, HALF), HALF)], taps, load.at[2]
        ),
        pltpu.make_async_copy(out_hbm.at[0], out, load.at[3]),
        pltpu.make_async_copy(query_hbm.at[0], query, load.at[4]),
        pltpu.make_async_copy(tab_hbm, tab_ref, load.at[5]),
        pltpu.make_async_copy(mid_hbm, mid_ref, load.at[6]),
        pltpu.make_async_copy(gain_hbm, gain_ref, load.at[7]),
    ]
    for copy in loads:
        copy.start()

    def greet(to_seq, to_ch):
        pl.semaphore_signal(barrier, inc=1, device_id=(to_seq, to_ch), device_id_type=MESH)

    with jax.named_scope("greet"):
        for_each_peer(greet, TURNS[::-1])

    def flip_product(left, right, target):
        def body(j, carry):
            cols = pl.ds(pl.multiple_of(j * BLOCK, BLOCK), BLOCK)
            target[cols, :] = (left[:, cols].astype(F32) * right[:, cols].astype(F32)).T
            return carry

        lax.fori_loop(0, WIDTH // BLOCK, body, 0)

    with jax.named_scope("load"):
        loads[0].wait()
        loads[1].wait()
    with jax.named_scope("flip_mixed"):
        flip_product(key, value, mixed_t)
    loads[2].wait()

    def flip_taps(j, carry):
        cols = pl.ds(pl.multiple_of(j * BLOCK, BLOCK), BLOCK)
        taps_t[cols, :] = taps[:, cols].astype(F32).T
        return carry

    with jax.named_scope("flip_taps"):
        lax.fori_loop(0, HALF // BLOCK, flip_taps, 0)
    with jax.named_scope("barrier"):
        pl.semaphore_wait(barrier, 2 * BLOCK - 1)
    with jax.named_scope("send_mixed"):
        send_all(mixed_t, mixed_in, send.at[0], recv.at[0])
    with jax.named_scope("send_taps"):
        send_same(taps_t, taps_in, send.at[1], recv.at[1])
    loads[3].wait()
    loads[4].wait()
    with jax.named_scope("flip_gated"):
        flip_product(out, query, gated_t)
    with jax.named_scope("send_gated"):
        send_all(gated_t, gated_in, send.at[2], recv.at[2])
    loads[5].wait()
    loads[6].wait()
    loads[7].wait()
    with jax.named_scope("wait_mixed"):
        wait_rows(mixed_in, ALL_ROWS, recv.at[0])
        wait_rows(taps_in, SAME_ROWS, recv.at[1])

    def conv_body(c, carry):
        tab, mid = tab_ref[...], mid_ref[...]
        parts = [mixed_in[channel_rows(b, c), :] for b in range(2)]
        parts.append(taps_in[channel_rows(0, c), :])
        mixed_a, mixed_b, taps_spec = to_spectrum(parts, tab, mid)
        t_re, t_im = taps_spec
        prods = []
        for b, (re, im) in enumerate((mixed_a, mixed_b)):
            mspec[c, b, 0] = re
            mspec[c, b, 1] = im
            prods.append((re * t_re - im * t_im, re * t_im + im * t_re))
        tspec[c, 0] = t_re
        tspec[c, 1] = t_im
        lines = from_spectrum(prods, tab, mid)
        for b in range(2):
            conv[channel_rows(b, c), :] = lines[b] * SCALE
        return carry

    with jax.named_scope("conv"):
        lax.fori_loop(0, OWNED, conv_body, 0)
    with jax.named_scope("send_conv"):
        send_all(conv, conv_in, send.at[3], recv.at[3])
    with jax.named_scope("wait_gated"):
        wait_rows(gated_in, ALL_ROWS, recv.at[2])

    def back_body(c, carry):
        tab, mid = tab_ref[...], mid_ref[...]
        gated = to_spectrum([gated_in[channel_rows(b, c), :] for b in range(2)], tab, mid)
        t_re, t_im = tspec[c, 0], tspec[c, 1]
        prods = []
        terms = []
        for b, (re, im) in enumerate(gated):
            m_re, m_im = mspec[c, b, 0], mspec[c, b, 1]
            prods.append((t_re * re + t_im * im, t_re * im - t_im * re))
            terms.append((m_re * re + m_im * im, m_re * im - m_im * re))
        prods.append((terms[0][0] + terms[1][0], terms[0][1] + terms[1][1]))
        lines = from_spectrum(prods, tab, mid)
        for b in range(2):
            back[channel_rows(b, c), :] = lines[b] * SCALE
        corr[channel_rows(0, c), :] = lines[2] * SCALE
        return carry

    with jax.named_scope("back"):
        lax.fori_loop(0, OWNED, back_body, 0)
    with jax.named_scope("send_back"):
        send_all(back, back_in, send.at[4], recv.at[4])
        send_same(corr, corr_in, send.at[5], recv.at[5], FAR_FIRST)

    with jax.named_scope("wait_conv"):
        wait_rows(conv_in, ALL_ROWS, recv.at[3])

    def query_body(j, carry):
        cols = pl.ds(pl.multiple_of(j * BLOCK, BLOCK), BLOCK)
        mixed = key[:, cols].astype(F32) * value[:, cols].astype(F32)
        full = conv_in[cols, :].T + gain_ref[:, cols] * mixed
        grad_query[0, :, cols] = (out[:, cols].astype(F32) * full).astype(BF16)
        return carry

    with jax.named_scope("query_out"):
        lax.fori_loop(0, WIDTH // BLOCK, query_body, 0)
    with jax.named_scope("wait_back"):
        wait_rows(back_in, ALL_ROWS, recv.at[4])

    def back_out(j, carry):
        cols = pl.ds(pl.multiple_of(j * BLOCK, BLOCK), BLOCK)
        gated = out[:, cols].astype(F32) * query[:, cols].astype(F32)
        full = back_in[cols, :].T + gain_ref[:, cols] * gated
        grad_key[0, :, cols] = (full * value[:, cols].astype(F32)).astype(BF16)
        grad_value[0, :, cols] = (full * key[:, cols].astype(F32)).astype(BF16)
        return carry

    with jax.named_scope("back_out"):
        lax.fori_loop(0, WIDTH // BLOCK, back_out, 0)
    with jax.named_scope("wait_corr"):
        wait_rows(corr_in, SAME_ROWS, recv.at[5])

    wait_rows(mixed_t, ALL_ROWS, send.at[0])
    wait_rows(taps_t, SAME_ROWS, send.at[1])
    wait_rows(gated_t, ALL_ROWS, send.at[2])
    wait_rows(conv, ALL_ROWS, send.at[3])
    wait_rows(back, ALL_ROWS, send.at[4])
    wait_rows(corr, SAME_ROWS, send.at[5])


def in_hbm(x):
    return pltpu.with_memory_space_constraint(x, pltpu.HBM)


def store_kernel(query, key, value, corr, to_query, to_key, to_value, to_filter, flipped, sems):
    pairs = ((query, to_query), (key, to_key), (value, to_value), (flipped, to_filter))
    copies = [pltpu.make_async_copy(*pair, sems.at[i]) for i, pair in enumerate(pairs)]
    for copy in copies[:3]:
        copy.start()
    for j in range(HALF // BLOCK):
        cols = slice(j * BLOCK, (j + 1) * BLOCK)
        flipped[:, cols] = corr[cols, :].T
    copies[3].start()
    for copy in copies:
        copy.wait()


def shards(query_gate, key_input, value_input, grad_output, filter_raw, skip_gain):
    tab, mid = tables()
    anywhere = pl.BlockSpec(memory_space=pltpu.HBM)
    vmem = pl.BlockSpec(memory_space=pltpu.VMEM)
    signal = pltpu.VMEM((1, BLOCK, WIDTH), BF16)
    narrow = pltpu.VMEM((BLOCK, WIDTH), BF16)
    tall = pltpu.VMEM((WIDTH, BLOCK), F32)
    short = pltpu.VMEM((HALF, BLOCK), F32)
    gain = skip_gain.reshape(1, WIDTH)
    arrays = (query_gate, key_input, value_input, grad_output, filter_raw, gain, tab, mid)
    operands = [in_hbm(x) for x in arrays]
    results = tuple(
        pl.pallas_call(
            kernel,
            out_shape=[signal, signal, signal, pltpu.VMEM((HALF, BLOCK), F32)],
            in_specs=[anywhere] * 8,
            out_specs=[vmem] * 4,
            scratch_shapes=[narrow] * 4
            + [
                pltpu.VMEM((BLOCK, HALF), BF16),
                pltpu.VMEM(tab.shape, BF16),
                pltpu.VMEM(mid.shape, F32),
                pltpu.VMEM((1, WIDTH), F32),
            ]
            + [tall, tall, short] * 3
            + [tall, tall]
            + [
                pltpu.VMEM((OWNED, 2, 2, BLOCK, BLOCK), F32),
                pltpu.VMEM((OWNED, 2, BLOCK, BLOCK), F32),
                pltpu.SemaphoreType.DMA((8,)),
                pltpu.SemaphoreType.DMA((6,)),
                pltpu.SemaphoreType.DMA((6,)),
            ],
            compiler_params=pltpu.CompilerParams(
                collective_id=0, has_side_effects=True, vmem_limit_bytes=32 * 1024 * 1024
            ),
            name="hyena_back",
        )(*operands)
    )
    return tuple(
        pl.pallas_call(
            store_kernel,
            out_shape=[jax.ShapeDtypeStruct(r.shape, r.dtype) for r in results[:3]]
            + [jax.ShapeDtypeStruct((BLOCK, HALF), F32)],
            in_specs=[vmem] * 4,
            out_specs=[anywhere] * 4,
            scratch_shapes=[
                pltpu.VMEM((BLOCK, HALF), F32),
                pltpu.SemaphoreType.DMA((4,)),
            ],
            compiler_params=pltpu.CompilerParams(vmem_limit_bytes=4 * 1024 * 1024),
            name="store",
        )(*results)
    )


def solution(mesh):
    in_specs = (
        P("ch", "seq", None),
        P("ch", "seq", None),
        P("ch", "seq", None),
        P("ch", "seq", None),
        P("seq", None),
        P(),
    )
    out_specs = (P("ch", "seq", None), P("ch", "seq", None), P("ch", "seq", None), P("seq", "ch"))
    return jax.shard_map(shards, mesh=mesh, in_specs=in_specs, out_specs=out_specs, check_vma=False)
```

```python
import itertools
import math

import jax
import jax.numpy as jnp
import numpy as np
from jax import lax
from jax.experimental import pallas as pl
from jax.experimental.pallas import tpu as pltpu
from jax.sharding import PartitionSpec as P

BLOCK = 128
FULL = 2 * BLOCK * BLOCK
F32 = jnp.float32
BF16 = jnp.bfloat16


def split_table(table):
    high = jnp.asarray(table, F32).astype(BF16)
    low = (jnp.asarray(table, F32) - high.astype(F32)).astype(BF16)
    return (high, low)


def tables():
    idx = np.arange(BLOCK)
    turn_one = 2.0 * math.pi / (2 * BLOCK) * ((idx[:, None] + 0.5) * idx[None, :])
    first = np.concatenate([np.cos(turn_one), -np.sin(turn_one)], axis=0)
    turn_two = 2.0 * math.pi / BLOCK * (idx[:, None] * idx[None, :] % BLOCK)
    cos_two, sin_two = np.cos(turn_two), np.sin(turn_two)
    second = np.block([[cos_two, -sin_two], [sin_two, cos_two]])
    second_inv = np.block([[cos_two, sin_two], [-sin_two, cos_two]])
    turn_mid = 2.0 * math.pi / FULL * ((idx[:, None] + 0.5) * idx[None, :])
    f_high, f_low = split_table(first.astype(np.float32))
    rows = [jnp.concatenate([f_high, f_low], axis=1)]
    for table in (second, second_inv, first.T):
        rows.extend(split_table(table.astype(np.float32)))
    mid = np.concatenate([np.cos(turn_mid), np.sin(turn_mid)], axis=0)
    return (jnp.concatenate(rows, axis=0), jnp.asarray(mid, F32))


def halves(x):
    high = x.astype(BF16)
    return (high, (x - high.astype(F32)).astype(BF16))


def dot(a, b):
    return jnp.dot(a, b, preferred_element_type=F32)


def dot_left(high, low, x):
    x_high, x_low = halves(x)
    return dot(high, x_high) + dot(low, x_high) + dot(high, x_low)


def dot_right(x, high, low):
    x_high, x_low = halves(x)
    return dot(x_high, high) + dot(x_high, low) + dot(x_low, high)


def to_spectrum(parts, tab, mid):
    cos_mid, sin_mid = mid[:BLOCK], mid[BLOCK:]
    lines = dot_left(tab[:256, :BLOCK], tab[:256, BLOCK:], jnp.concatenate(parts, axis=1))
    rows = []
    for i in range(len(parts)):
        re = lines[:BLOCK, i * BLOCK : (i + 1) * BLOCK]
        im = lines[BLOCK:, i * BLOCK : (i + 1) * BLOCK]
        rows.append(
            jnp.concatenate([re * cos_mid + im * sin_mid, im * cos_mid - re * sin_mid], axis=1)
        )
    spec = dot_right(jnp.concatenate(rows, axis=0), tab[256:512], tab[512:768])
    return [
        (spec[i * BLOCK : (i + 1) * BLOCK, :BLOCK], spec[i * BLOCK : (i + 1) * BLOCK, BLOCK:])
        for i in range(len(parts))
    ]


def from_spectrum(specs, tab, mid):
    cos_mid, sin_mid = mid[:BLOCK], mid[BLOCK:]
    rows = jnp.concatenate([jnp.concatenate([re, im], axis=1) for re, im in specs], axis=0)
    grid = dot_right(rows, tab[768:1024], tab[1024:1280])
    cols = []
    for i in range(len(specs)):
        re = grid[i * BLOCK : (i + 1) * BLOCK, :BLOCK]
        im = grid[i * BLOCK : (i + 1) * BLOCK, BLOCK:]
        cols.append(
            jnp.concatenate([re * cos_mid - im * sin_mid, im * cos_mid + re * sin_mid], axis=0)
        )
    lines = dot_left(tab[1280:1408], tab[1408:1536], jnp.concatenate(cols, axis=1))
    return [lines[:, i * BLOCK : (i + 1) * BLOCK] for i in range(len(specs))]


SCALE = 1.0 / (BLOCK * (FULL // 2))
OWNED = 8
WIDTH = 2048
HALF = WIDTH // 2
MESH = pl.DeviceIdType.MESH


def channel_rows(part, channel):
    return pl.ds(part * BLOCK * OWNED + channel, BLOCK, stride=OWNED)


def tile(index):
    return pl.ds(pl.multiple_of(index * OWNED, OWNED), OWNED)


TURNS = (0, 1, 7, 2, 6, 3, 5, 4)
SLAB = BLOCK // 8


def ring_bases(turns=TURNS):
    z = lax.div(lax.axis_index("seq"), SLAB)
    return [lax.rem(z + turn, 8) * SLAB for turn in turns]


def at_step(step):
    place = lax.rem(lax.axis_index("seq"), SLAB) * 2 + lax.axis_index("ch")
    rest = lax.rem(place + step, 2 * SLAB)
    return (lax.div(rest, 2), lax.rem(rest, 2))


def for_each_peer(visit):
    bases = ring_bases()

    def body(step, carry):
        low, to_ch = at_step(step)
        for base in bases:
            visit(base + low, to_ch)
        return carry

    low, to_ch = at_step(0)
    for base in bases[1:]:
        visit(base + low, to_ch)
    lax.fori_loop(1, 2 * SLAB, body, 0)


def hops(move):
    z, x, y, core = move
    return (min(z, 8 - z) + 2 * x + min(y, 4 - y), core)


MOVES = sorted(itertools.product(range(8), range(2), range(4), range(2)), key=hops)[:0:-1]


def for_each_same(visit):
    seq = lax.axis_index("seq")
    z, x = lax.div(seq, SLAB), lax.rem(lax.div(seq, 8), 2)
    y, core = lax.rem(lax.div(seq, 2), 4), lax.rem(seq, 2)
    zs = [lax.rem(z + i, 8) * SLAB for i in range(8)]
    xs = [lax.rem(x + i, 2) * 8 for i in range(2)]
    ys = [lax.rem(y + i, 4) * 2 for i in range(4)]
    cores = [core, 1 - core]
    for move in MOVES:
        visit(zs[move[0]] + xs[move[1]] + ys[move[2]] + cores[move[3]])


def tile_sender(source, target, send, recv):
    me = lax.axis_index("ch") * BLOCK + lax.axis_index("seq")

    def visit(to_seq, to_ch):
        pltpu.make_async_remote_copy(
            src_ref=source.at[tile(to_ch * BLOCK + to_seq)],
            dst_ref=target.at[tile(me)],
            send_sem=send,
            recv_sem=recv,
            device_id=(to_seq, to_ch),
            device_id_type=MESH,
        ).start()

    return visit


def keep_own(source, target):
    me = lax.axis_index("ch") * BLOCK + lax.axis_index("seq")
    target[tile(me), :] = source[tile(me), :]


def send_all(source, target, send, recv):
    for_each_peer(tile_sender(source, target, send, recv))
    keep_own(source, target)


def send_same(source, target, send, recv):
    seq, ch = lax.axis_index("seq"), lax.axis_index("ch")

    def visit(to_seq):
        pltpu.make_async_remote_copy(
            src_ref=source.at[tile(to_seq)],
            dst_ref=target.at[tile(seq)],
            send_sem=send,
            recv_sem=recv,
            device_id=(to_seq, ch),
            device_id_type=MESH,
        ).start()

    for_each_same(visit)
    target[tile(seq), :] = source[tile(seq), :]


def wait_rows(ref, rows, sem):
    part = ref.at[pl.ds(0, rows)]
    pltpu.make_async_copy(part, part, sem).wait()


ALL_ROWS = WIDTH - OWNED
SAME_ROWS = HALF - OWNED


def kernel(
    query_hbm,
    key_hbm,
    value_hbm,
    out_hbm,
    filter_hbm,
    gain_hbm,
    tab_hbm,
    mid_hbm,
    grad_query,
    grad_key,
    grad_value,
    corr_in,
    query,
    key,
    value,
    out,
    taps,
    tab_ref,
    mid_ref,
    gain_ref,
    mixed_t,
    gated_t,
    taps_t,
    mixed_in,
    gated_in,
    taps_in,
    conv,
    back,
    corr,
    conv_in,
    back_in,
    mspec,
    tspec,
    load,
    send,
    recv,
    ready,
):
    seq, ch = lax.axis_index("seq"), lax.axis_index("ch")
    barrier = pltpu.get_barrier_semaphore()

    def own_half(ref):
        return ref.at[:, pl.ds(pl.multiple_of(ch * HALF, HALF), HALF)]

    def other_half(ref):
        return ref.at[:, pl.ds(pl.multiple_of((1 - ch) * HALF, HALF), HALF)]

    key_src, value_src = key_hbm.at[0], value_hbm.at[0]
    loads = [
        pltpu.make_async_copy(own_half(key_src), own_half(key), load.at[0]),
        pltpu.make_async_copy(own_half(value_src), own_half(value), load.at[1]),
        pltpu.make_async_copy(other_half(key_src), other_half(key), load.at[2]),
        pltpu.make_async_copy(other_half(value_src), other_half(value), load.at[3]),
        pltpu.make_async_copy(own_half(filter_hbm), taps, load.at[4]),
        pltpu.make_async_copy(out_hbm.at[0], out, load.at[5]),
        pltpu.make_async_copy(query_hbm.at[0], query, load.at[6]),
        pltpu.make_async_copy(tab_hbm, tab_ref, load.at[7]),
        pltpu.make_async_copy(mid_hbm, mid_ref, load.at[8]),
        pltpu.make_async_copy(gain_hbm, gain_ref, load.at[9]),
    ]
    for copy in loads[:4]:
        copy.start()

    bases = ring_bases()

    def greet(to_seq, to_ch):
        pl.semaphore_signal(barrier, inc=1, device_id=(to_seq, to_ch), device_id_type=MESH)

    with jax.named_scope("greet"):
        for base in bases[:0:-1]:
            greet(base + lax.rem(seq, SLAB), ch)
        for step in range(2 * SLAB - 1, 0, -1):
            low, to_ch = at_step(step)
            greet(bases[0] + low, to_ch)
        for copy in loads[4:]:
            copy.start()

    def flip_product(left, right, target, first=0, count=WIDTH // BLOCK):
        def body(j, carry):
            cols = pl.ds(pl.multiple_of(first + j * BLOCK, BLOCK), BLOCK)
            target[cols, :] = (left[:, cols].astype(F32) * right[:, cols].astype(F32)).T
            return carry

        lax.fori_loop(0, count, body, 0)

    def flip_taps(j, carry):
        cols = pl.ds(pl.multiple_of(j * BLOCK, BLOCK), BLOCK)
        taps_t[cols, :] = taps[:, cols].astype(F32).T
        return carry

    send_mixed = tile_sender(mixed_t, mixed_in, send.at[0], recv.at[0])

    def mixed_step(step):
        low, to_ch = at_step(step)
        pl.semaphore_wait(ready.at[2 * low + to_ch], 1)
        for base in bases:
            send_mixed(base + low, to_ch)

    def mixed_even(i, carry):
        mixed_step(2 * i)
        return carry

    def mixed_odd(i, carry):
        mixed_step(2 * i + 1)
        return carry

    with jax.named_scope("barrier"):
        pl.semaphore_wait(barrier, 7 + 2 * SLAB - 1)
        mine = ready.at[2 * lax.rem(seq, SLAB) + ch]
        for step in range(1, 2 * SLAB):
            low, to_ch = at_step(step)
            pl.semaphore_signal(
                mine, inc=1, device_id=(bases[0] + low, to_ch), device_id_type=MESH
            )
    with jax.named_scope("load"):
        loads[0].wait()
        loads[1].wait()
    with jax.named_scope("flip_mixed"):
        flip_product(key, value, mixed_t, ch * HALF, HALF // BLOCK)
    with jax.named_scope("send_mixed"):
        for base in bases[1:]:
            send_mixed(base + lax.rem(seq, SLAB), ch)
        lax.fori_loop(1, SLAB, mixed_even, 0)
    with jax.named_scope("flip_mixed2"):
        loads[2].wait()
        loads[3].wait()
        flip_product(key, value, mixed_t, (1 - ch) * HALF, HALF // BLOCK)
    with jax.named_scope("send_mixed2"):
        lax.fori_loop(0, SLAB, mixed_odd, 0)
        keep_own(mixed_t, mixed_in)
    with jax.named_scope("flip_taps"):
        loads[4].wait()
        lax.fori_loop(0, HALF // BLOCK, flip_taps, 0)
    with jax.named_scope("send_taps"):
        send_same(taps_t, taps_in, send.at[1], recv.at[1])
    loads[5].wait()
    loads[6].wait()
    with jax.named_scope("flip_gated"):
        flip_product(out, query, gated_t)
    with jax.named_scope("send_gated"):
        send_all(gated_t, gated_in, send.at[2], recv.at[2])
    for copy in loads[7:]:
        copy.wait()
    with jax.named_scope("wait_mixed"):
        wait_rows(mixed_in, ALL_ROWS, recv.at[0])
        wait_rows(taps_in, SAME_ROWS, recv.at[1])

    def conv_body(c, carry):
        tab, mid = tab_ref[...], mid_ref[...]
        parts = [mixed_in[channel_rows(b, c), :] for b in range(2)]
        parts.append(taps_in[channel_rows(0, c), :])
        mixed_a, mixed_b, taps_spec = to_spectrum(parts, tab, mid)
        t_re, t_im = taps_spec
        prods = []
        for b, (re, im) in enumerate((mixed_a, mixed_b)):
            mspec[c, b, 0] = re
            mspec[c, b, 1] = im
            prods.append((re * t_re - im * t_im, re * t_im + im * t_re))
        tspec[c, 0] = t_re
        tspec[c, 1] = t_im
        lines = from_spectrum(prods, tab, mid)
        for b in range(2):
            conv[channel_rows(b, c), :] = lines[b] * SCALE
        return carry

    with jax.named_scope("conv"):
        lax.fori_loop(0, OWNED, conv_body, 0)
    with jax.named_scope("send_conv"):
        send_all(conv, conv_in, send.at[3], recv.at[3])
    with jax.named_scope("wait_gated"):
        wait_rows(gated_in, ALL_ROWS, recv.at[2])

    def back_body(c, carry):
        tab, mid = tab_ref[...], mid_ref[...]
        gated = to_spectrum([gated_in[channel_rows(b, c), :] for b in range(2)], tab, mid)
        t_re, t_im = tspec[c, 0], tspec[c, 1]
        prods = []
        terms = []
        for b, (re, im) in enumerate(gated):
            m_re, m_im = mspec[c, b, 0], mspec[c, b, 1]
            prods.append((t_re * re + t_im * im, t_re * im - t_im * re))
            terms.append((m_re * re + m_im * im, m_re * im - m_im * re))
        prods.append((terms[0][0] + terms[1][0], terms[0][1] + terms[1][1]))
        lines = from_spectrum(prods, tab, mid)
        for b in range(2):
            back[channel_rows(b, c), :] = lines[b] * SCALE
        corr[channel_rows(0, c), :] = lines[2] * SCALE
        return carry

    with jax.named_scope("back"):
        lax.fori_loop(0, OWNED, back_body, 0)
    with jax.named_scope("send_back"):
        send_all(back, back_in, send.at[4], recv.at[4])
        send_same(corr, corr_in, send.at[5], recv.at[5])

    with jax.named_scope("wait_conv"):
        wait_rows(conv_in, ALL_ROWS, recv.at[3])

    def query_body(j, carry):
        cols = pl.ds(pl.multiple_of(j * BLOCK, BLOCK), BLOCK)
        mixed = key[:, cols].astype(F32) * value[:, cols].astype(F32)
        full = conv_in[cols, :].T + gain_ref[:, cols] * mixed
        grad_query[0, :, cols] = (out[:, cols].astype(F32) * full).astype(BF16)
        return carry

    with jax.named_scope("query_out"):
        lax.fori_loop(0, WIDTH // BLOCK, query_body, 0)
    with jax.named_scope("wait_back"):
        wait_rows(back_in, ALL_ROWS, recv.at[4])

    def back_out(j, carry):
        cols = pl.ds(pl.multiple_of(j * BLOCK, BLOCK), BLOCK)
        gated = out[:, cols].astype(F32) * query[:, cols].astype(F32)
        full = back_in[cols, :].T + gain_ref[:, cols] * gated
        grad_key[0, :, cols] = (full * value[:, cols].astype(F32)).astype(BF16)
        grad_value[0, :, cols] = (full * key[:, cols].astype(F32)).astype(BF16)
        return carry

    with jax.named_scope("back_out"):
        lax.fori_loop(0, WIDTH // BLOCK, back_out, 0)
    with jax.named_scope("wait_corr"):
        wait_rows(corr_in, SAME_ROWS, recv.at[5])
    wait_rows(mixed_t, ALL_ROWS, send.at[0])
    wait_rows(taps_t, SAME_ROWS, send.at[1])
    wait_rows(gated_t, ALL_ROWS, send.at[2])
    wait_rows(conv, ALL_ROWS, send.at[3])
    wait_rows(back, ALL_ROWS, send.at[4])
    wait_rows(corr, SAME_ROWS, send.at[5])


def in_hbm(x):
    return pltpu.with_memory_space_constraint(x, pltpu.HBM)


def store_kernel(query, key, value, corr, to_query, to_key, to_value, to_filter, flipped, sems):
    pairs = ((query, to_query), (key, to_key), (value, to_value), (flipped, to_filter))
    copies = [pltpu.make_async_copy(*pair, sems.at[i]) for i, pair in enumerate(pairs)]
    for copy in copies[:3]:
        copy.start()
    for j in range(HALF // BLOCK):
        cols = slice(j * BLOCK, (j + 1) * BLOCK)
        flipped[:, cols] = corr[cols, :].T
    copies[3].start()
    for copy in copies:
        copy.wait()


def shards(query_gate, key_input, value_input, grad_output, filter_raw, skip_gain):
    tab, mid = tables()
    anywhere = pl.BlockSpec(memory_space=pltpu.HBM)
    vmem = pl.BlockSpec(memory_space=pltpu.VMEM)
    signal = pltpu.VMEM((1, BLOCK, WIDTH), BF16)
    narrow = pltpu.VMEM((BLOCK, WIDTH), BF16)
    tall = pltpu.VMEM((WIDTH, BLOCK), F32)
    short = pltpu.VMEM((HALF, BLOCK), F32)
    gain = skip_gain.reshape(1, WIDTH)
    arrays = (query_gate, key_input, value_input, grad_output, filter_raw, gain, tab, mid)
    operands = [in_hbm(x) for x in arrays]
    results = tuple(
        pl.pallas_call(
            kernel,
            out_shape=[signal, signal, signal, pltpu.VMEM((HALF, BLOCK), F32)],
            in_specs=[anywhere] * 8,
            out_specs=[vmem] * 4,
            scratch_shapes=[narrow] * 4
            + [
                pltpu.VMEM((BLOCK, HALF), BF16),
                pltpu.VMEM(tab.shape, BF16),
                pltpu.VMEM(mid.shape, F32),
                pltpu.VMEM((1, WIDTH), F32),
            ]
            + [tall, tall, short] * 3
            + [tall, tall]
            + [
                pltpu.VMEM((OWNED, 2, 2, BLOCK, BLOCK), F32),
                pltpu.VMEM((OWNED, 2, BLOCK, BLOCK), F32),
                pltpu.SemaphoreType.DMA((10,)),
                pltpu.SemaphoreType.DMA((6,)),
                pltpu.SemaphoreType.DMA((6,)),
                pltpu.SemaphoreType.REGULAR((2 * SLAB,)),
            ],
            compiler_params=pltpu.CompilerParams(
                collective_id=0, has_side_effects=True, vmem_limit_bytes=32 * 1024 * 1024
            ),
            name="hyena_back",
        )(*operands)
    )
    return tuple(
        pl.pallas_call(
            store_kernel,
            out_shape=[jax.ShapeDtypeStruct(r.shape, r.dtype) for r in results[:3]]
            + [jax.ShapeDtypeStruct((BLOCK, HALF), F32)],
            in_specs=[vmem] * 4,
            out_specs=[anywhere] * 4,
            scratch_shapes=[
                pltpu.VMEM((BLOCK, HALF), F32),
                pltpu.SemaphoreType.DMA((4,)),
            ],
            compiler_params=pltpu.CompilerParams(vmem_limit_bytes=4 * 1024 * 1024),
            name="store",
        )(*results)
    )


def solution(mesh):
    in_specs = (
        P("ch", "seq", None),
        P("ch", "seq", None),
        P("ch", "seq", None),
        P("ch", "seq", None),
        P("seq", None),
        P(),
    )
    out_specs = (P("ch", "seq", None), P("ch", "seq", None), P("ch", "seq", None), P("seq", "ch"))
    return jax.shard_map(shards, mesh=mesh, in_specs=in_specs, out_specs=out_specs, check_vma=False)
```

```python
import itertools
import math

import jax
import jax.numpy as jnp
import numpy as np
from jax import lax
from jax.experimental import pallas as pl
from jax.experimental.pallas import tpu as pltpu
from jax.sharding import PartitionSpec as P

BLOCK = 128
FULL = 2 * BLOCK * BLOCK
F32 = jnp.float32
BF16 = jnp.bfloat16


def split_table(table):
    high = jnp.asarray(table, F32).astype(BF16)
    low = (jnp.asarray(table, F32) - high.astype(F32)).astype(BF16)
    return (high, low)


def tables():
    idx = np.arange(BLOCK)
    turn_one = 2.0 * math.pi / (2 * BLOCK) * ((idx[:, None] + 0.5) * idx[None, :])
    first = np.concatenate([np.cos(turn_one), -np.sin(turn_one)], axis=0)
    turn_two = 2.0 * math.pi / BLOCK * (idx[:, None] * idx[None, :] % BLOCK)
    cos_two, sin_two = np.cos(turn_two), np.sin(turn_two)
    second = np.block([[cos_two, -sin_two], [sin_two, cos_two]])
    second_inv = np.block([[cos_two, sin_two], [-sin_two, cos_two]])
    turn_mid = 2.0 * math.pi / FULL * ((idx[:, None] + 0.5) * idx[None, :])
    f_high, f_low = split_table(first.astype(np.float32))
    rows = [jnp.concatenate([f_high, f_low], axis=1)]
    for table in (second, second_inv, first.T):
        rows.extend(split_table(table.astype(np.float32)))
    mid = np.concatenate([np.cos(turn_mid), np.sin(turn_mid)], axis=0)
    return (jnp.concatenate(rows, axis=0), jnp.asarray(mid, F32))


def halves(x):
    high = x.astype(BF16)
    return (high, (x - high.astype(F32)).astype(BF16))


def dot(a, b):
    return jnp.dot(a, b, preferred_element_type=F32)


def dot_left(high, low, x):
    x_high, x_low = halves(x)
    return dot(high, x_high) + dot(low, x_high) + dot(high, x_low)


def dot_right(x, high, low):
    x_high, x_low = halves(x)
    return dot(x_high, high) + dot(x_high, low) + dot(x_low, high)


def to_spectrum(parts, tab, mid):
    cos_mid, sin_mid = mid[:BLOCK], mid[BLOCK:]
    lines = dot_left(tab[:256, :BLOCK], tab[:256, BLOCK:], jnp.concatenate(parts, axis=1))
    rows = []
    for i in range(len(parts)):
        re = lines[:BLOCK, i * BLOCK : (i + 1) * BLOCK]
        im = lines[BLOCK:, i * BLOCK : (i + 1) * BLOCK]
        rows.append(
            jnp.concatenate([re * cos_mid + im * sin_mid, im * cos_mid - re * sin_mid], axis=1)
        )
    spec = dot_right(jnp.concatenate(rows, axis=0), tab[256:512], tab[512:768])
    return [
        (spec[i * BLOCK : (i + 1) * BLOCK, :BLOCK], spec[i * BLOCK : (i + 1) * BLOCK, BLOCK:])
        for i in range(len(parts))
    ]


def from_spectrum(specs, tab, mid):
    cos_mid, sin_mid = mid[:BLOCK], mid[BLOCK:]
    rows = jnp.concatenate([jnp.concatenate([re, im], axis=1) for re, im in specs], axis=0)
    grid = dot_right(rows, tab[768:1024], tab[1024:1280])
    cols = []
    for i in range(len(specs)):
        re = grid[i * BLOCK : (i + 1) * BLOCK, :BLOCK]
        im = grid[i * BLOCK : (i + 1) * BLOCK, BLOCK:]
        cols.append(
            jnp.concatenate([re * cos_mid - im * sin_mid, im * cos_mid + re * sin_mid], axis=0)
        )
    lines = dot_left(tab[1280:1408], tab[1408:1536], jnp.concatenate(cols, axis=1))
    return [lines[:, i * BLOCK : (i + 1) * BLOCK] for i in range(len(specs))]


SCALE = 1.0 / (BLOCK * (FULL // 2))
OWNED = 8
WIDTH = 2048
HALF = WIDTH // 2
MESH = pl.DeviceIdType.MESH


def channel_rows(part, channel):
    return pl.ds(part * BLOCK * OWNED + channel, BLOCK, stride=OWNED)


def tile(index):
    return pl.ds(pl.multiple_of(index * OWNED, OWNED), OWNED)


TURNS = (0, 1, 7, 2, 6, 3, 5, 4)
SLAB = BLOCK // 8


def ring_bases(turns=TURNS):
    z = lax.div(lax.axis_index("seq"), SLAB)
    return [lax.rem(z + turn, 8) * SLAB for turn in turns]


def at_step(step):
    place = lax.rem(lax.axis_index("seq"), SLAB) * 2 + lax.axis_index("ch")
    rest = lax.rem(place + step, 2 * SLAB)
    return (lax.div(rest, 2), lax.rem(rest, 2))


def for_each_peer(visit):
    bases = ring_bases()

    def body(step, carry):
        low, to_ch = at_step(step)
        for base in bases:
            visit(base + low, to_ch)
        return carry

    low, to_ch = at_step(0)
    for base in bases[1:]:
        visit(base + low, to_ch)
    lax.fori_loop(1, 2 * SLAB, body, 0)


def hops(move):
    z, x, y, core = move
    return (2 * x + min(y, 4 - y) + core, min(z, 8 - z))


MOVES = sorted(itertools.product(range(8), range(2), range(4), range(2)), key=hops)[:0:-1]


def hops_all(move):
    z, x, y, core = move
    return (min(x, 4 - x) + min(y, 4 - y) + core, min(z, 8 - z))


MOVES_ALL = sorted(itertools.product(range(8), range(4), range(4), range(2)), key=hops_all)[:0:-1]


def for_each_far(visit):
    seq, ch = lax.axis_index("seq"), lax.axis_index("ch")
    z, x = lax.div(seq, SLAB), lax.rem(lax.div(seq, 8), 2) * 2 + ch
    y, core = lax.rem(lax.div(seq, 2), 4), lax.rem(seq, 2)
    zs = [lax.rem(z + i, 8) * SLAB for i in range(8)]
    xs = [lax.rem(x + i, 4) for i in range(4)]
    highs, lows = [lax.div(i, 2) * 8 for i in xs], [lax.rem(i, 2) for i in xs]
    ys = [lax.rem(y + i, 4) * 2 for i in range(4)]
    cores = [core, 1 - core]
    for move in MOVES_ALL:
        visit(zs[move[0]] + highs[move[1]] + ys[move[2]] + cores[move[3]], lows[move[1]])


def for_each_same(visit):
    seq = lax.axis_index("seq")
    z, x = lax.div(seq, SLAB), lax.rem(lax.div(seq, 8), 2)
    y, core = lax.rem(lax.div(seq, 2), 4), lax.rem(seq, 2)
    zs = [lax.rem(z + i, 8) * SLAB for i in range(8)]
    xs = [lax.rem(x + i, 2) * 8 for i in range(2)]
    ys = [lax.rem(y + i, 4) * 2 for i in range(4)]
    cores = [core, 1 - core]
    for move in MOVES:
        visit(zs[move[0]] + xs[move[1]] + ys[move[2]] + cores[move[3]])


def tile_sender(source, target, send, recv):
    me = lax.axis_index("ch") * BLOCK + lax.axis_index("seq")

    def visit(to_seq, to_ch):
        pltpu.make_async_remote_copy(
            src_ref=source.at[tile(to_ch * BLOCK + to_seq)],
            dst_ref=target.at[tile(me)],
            send_sem=send,
            recv_sem=recv,
            device_id=(to_seq, to_ch),
            device_id_type=MESH,
        ).start()

    return visit


def keep_own(source, target):
    me = lax.axis_index("ch") * BLOCK + lax.axis_index("seq")
    target[tile(me), :] = source[tile(me), :]


def send_all(source, target, send, recv, visits=None):
    (visits or for_each_peer)(tile_sender(source, target, send, recv))
    keep_own(source, target)


def send_same(source, target, send, recv):
    seq, ch = lax.axis_index("seq"), lax.axis_index("ch")

    def visit(to_seq):
        pltpu.make_async_remote_copy(
            src_ref=source.at[tile(to_seq)],
            dst_ref=target.at[tile(seq)],
            send_sem=send,
            recv_sem=recv,
            device_id=(to_seq, ch),
            device_id_type=MESH,
        ).start()

    for_each_same(visit)
    target[tile(seq), :] = source[tile(seq), :]


def wait_rows(ref, rows, sem):
    part = ref.at[pl.ds(0, rows)]
    pltpu.make_async_copy(part, part, sem).wait()


ALL_ROWS = WIDTH - OWNED
SAME_ROWS = HALF - OWNED


def kernel(
    query_hbm,
    key_hbm,
    value_hbm,
    out_hbm,
    filter_hbm,
    gain_hbm,
    tab_hbm,
    mid_hbm,
    grad_query,
    grad_key,
    grad_value,
    corr_in,
    query,
    key,
    value,
    out,
    taps,
    tab_ref,
    mid_ref,
    gain_ref,
    mixed_t,
    gated_t,
    taps_t,
    mixed_in,
    gated_in,
    taps_in,
    conv,
    back,
    corr,
    conv_in,
    back_in,
    mspec,
    tspec,
    load,
    send,
    recv,
    ready,
):
    seq, ch = lax.axis_index("seq"), lax.axis_index("ch")
    barrier = pltpu.get_barrier_semaphore()

    def own_half(ref):
        return ref.at[:, pl.ds(pl.multiple_of(ch * HALF, HALF), HALF)]

    def other_half(ref):
        return ref.at[:, pl.ds(pl.multiple_of((1 - ch) * HALF, HALF), HALF)]

    key_src, value_src = key_hbm.at[0], value_hbm.at[0]
    loads = [
        pltpu.make_async_copy(own_half(key_src), own_half(key), load.at[0]),
        pltpu.make_async_copy(own_half(value_src), own_half(value), load.at[1]),
        pltpu.make_async_copy(other_half(key_src), other_half(key), load.at[2]),
        pltpu.make_async_copy(other_half(value_src), other_half(value), load.at[3]),
        pltpu.make_async_copy(own_half(filter_hbm), taps, load.at[4]),
        pltpu.make_async_copy(out_hbm.at[0], out, load.at[5]),
        pltpu.make_async_copy(query_hbm.at[0], query, load.at[6]),
        pltpu.make_async_copy(tab_hbm, tab_ref, load.at[7]),
        pltpu.make_async_copy(mid_hbm, mid_ref, load.at[8]),
        pltpu.make_async_copy(gain_hbm, gain_ref, load.at[9]),
    ]
    for copy in loads[:4]:
        copy.start()

    bases = ring_bases()

    def greet(to_seq, to_ch):
        pl.semaphore_signal(barrier, inc=1, device_id=(to_seq, to_ch), device_id_type=MESH)

    with jax.named_scope("greet"):
        for base in bases[:0:-1]:
            greet(base + lax.rem(seq, SLAB), ch)
        for step in range(2 * SLAB - 1, 0, -1):
            low, to_ch = at_step(step)
            greet(bases[0] + low, to_ch)
        for copy in loads[4:]:
            copy.start()

    def flip_product(left, right, target, first=0, count=WIDTH // BLOCK):
        def body(j, carry):
            cols = pl.ds(pl.multiple_of(first + j * BLOCK, BLOCK), BLOCK)
            target[cols, :] = (left[:, cols].astype(F32) * right[:, cols].astype(F32)).T
            return carry

        lax.fori_loop(0, count, body, 0)

    def flip_taps(j, carry):
        cols = pl.ds(pl.multiple_of(j * BLOCK, BLOCK), BLOCK)
        taps_t[cols, :] = taps[:, cols].astype(F32).T
        return carry

    send_mixed = tile_sender(mixed_t, mixed_in, send.at[0], recv.at[0])

    def mixed_step(step):
        low, to_ch = at_step(step)
        pl.semaphore_wait(ready.at[2 * low + to_ch], 1)
        for base in bases:
            send_mixed(base + low, to_ch)

    def mixed_even(i, carry):
        mixed_step(2 * i)
        return carry

    def mixed_odd(i, carry):
        mixed_step(2 * i + 1)
        return carry

    with jax.named_scope("barrier"):
        pl.semaphore_wait(barrier, 7 + 2 * SLAB - 1)
        mine = ready.at[2 * lax.rem(seq, SLAB) + ch]
        for step in range(1, 2 * SLAB):
            low, to_ch = at_step(step)
            pl.semaphore_signal(
                mine, inc=1, device_id=(bases[0] + low, to_ch), device_id_type=MESH
            )
    with jax.named_scope("load"):
        loads[0].wait()
        loads[1].wait()
    with jax.named_scope("flip_mixed"):
        flip_product(key, value, mixed_t, ch * HALF, HALF // BLOCK)
    with jax.named_scope("send_mixed"):
        for base in bases[1:]:
            send_mixed(base + lax.rem(seq, SLAB), ch)
        lax.fori_loop(1, SLAB, mixed_even, 0)
    with jax.named_scope("flip_mixed2"):
        loads[2].wait()
        loads[3].wait()
        flip_product(key, value, mixed_t, (1 - ch) * HALF, HALF // BLOCK)
    with jax.named_scope("send_mixed2"):
        lax.fori_loop(0, SLAB, mixed_odd, 0)
        keep_own(mixed_t, mixed_in)
    with jax.named_scope("flip_taps"):
        loads[4].wait()
        lax.fori_loop(0, HALF // BLOCK, flip_taps, 0)
    with jax.named_scope("send_taps"):
        send_same(taps_t, taps_in, send.at[1], recv.at[1])
    loads[5].wait()
    loads[6].wait()
    with jax.named_scope("flip_gated"):
        flip_product(out, query, gated_t)
    with jax.named_scope("send_gated"):
        send_all(gated_t, gated_in, send.at[2], recv.at[2])
    for copy in loads[7:]:
        copy.wait()
    with jax.named_scope("wait_mixed"):
        wait_rows(mixed_in, ALL_ROWS, recv.at[0])
        wait_rows(taps_in, SAME_ROWS, recv.at[1])

    def conv_body(c, carry):
        tab, mid = tab_ref[...], mid_ref[...]
        parts = [mixed_in[channel_rows(b, c), :] for b in range(2)]
        parts.append(taps_in[channel_rows(0, c), :])
        mixed_a, mixed_b, taps_spec = to_spectrum(parts, tab, mid)
        t_re, t_im = taps_spec
        prods = []
        for b, (re, im) in enumerate((mixed_a, mixed_b)):
            mspec[c, b, 0] = re
            mspec[c, b, 1] = im
            prods.append((re * t_re - im * t_im, re * t_im + im * t_re))
        tspec[c, 0] = t_re
        tspec[c, 1] = t_im
        lines = from_spectrum(prods, tab, mid)
        for b in range(2):
            conv[channel_rows(b, c), :] = lines[b] * SCALE
        return carry

    with jax.named_scope("conv"):
        lax.fori_loop(0, OWNED, conv_body, 0)
    with jax.named_scope("send_conv"):
        send_all(conv, conv_in, send.at[3], recv.at[3])
    with jax.named_scope("wait_gated"):
        wait_rows(gated_in, ALL_ROWS, recv.at[2])

    def back_body(c, carry):
        tab, mid = tab_ref[...], mid_ref[...]
        gated = to_spectrum([gated_in[channel_rows(b, c), :] for b in range(2)], tab, mid)
        t_re, t_im = tspec[c, 0], tspec[c, 1]
        prods = []
        terms = []
        for b, (re, im) in enumerate(gated):
            m_re, m_im = mspec[c, b, 0], mspec[c, b, 1]
            prods.append((t_re * re + t_im * im, t_re * im - t_im * re))
            terms.append((m_re * re + m_im * im, m_re * im - m_im * re))
        prods.append((terms[0][0] + terms[1][0], terms[0][1] + terms[1][1]))
        lines = from_spectrum(prods, tab, mid)
        for b in range(2):
            back[channel_rows(b, c), :] = lines[b] * SCALE
        corr[channel_rows(0, c), :] = lines[2] * SCALE
        return carry

    with jax.named_scope("back"):
        lax.fori_loop(0, OWNED, back_body, 0)
    with jax.named_scope("send_back"):
        send_all(back, back_in, send.at[4], recv.at[4], for_each_far)
        send_same(corr, corr_in, send.at[5], recv.at[5])

    with jax.named_scope("wait_conv"):
        wait_rows(conv_in, ALL_ROWS, recv.at[3])

    def query_body(j, carry):
        cols = pl.ds(pl.multiple_of(j * BLOCK, BLOCK), BLOCK)
        mixed = key[:, cols].astype(F32) * value[:, cols].astype(F32)
        full = conv_in[cols, :].T + gain_ref[:, cols] * mixed
        grad_query[0, :, cols] = (out[:, cols].astype(F32) * full).astype(BF16)
        return carry

    with jax.named_scope("query_out"):
        lax.fori_loop(0, WIDTH // BLOCK, query_body, 0)
    with jax.named_scope("wait_back"):
        wait_rows(back_in, ALL_ROWS, recv.at[4])

    def back_out(j, carry):
        cols = pl.ds(pl.multiple_of(j * BLOCK, BLOCK), BLOCK)
        gated = out[:, cols].astype(F32) * query[:, cols].astype(F32)
        full = back_in[cols, :].T + gain_ref[:, cols] * gated
        grad_key[0, :, cols] = (full * value[:, cols].astype(F32)).astype(BF16)
        grad_value[0, :, cols] = (full * key[:, cols].astype(F32)).astype(BF16)
        return carry

    with jax.named_scope("back_out"):
        lax.fori_loop(0, WIDTH // BLOCK, back_out, 0)
    with jax.named_scope("wait_corr"):
        wait_rows(corr_in, SAME_ROWS, recv.at[5])
    wait_rows(mixed_t, ALL_ROWS, send.at[0])
    wait_rows(taps_t, SAME_ROWS, send.at[1])
    wait_rows(gated_t, ALL_ROWS, send.at[2])
    wait_rows(conv, ALL_ROWS, send.at[3])
    wait_rows(back, ALL_ROWS, send.at[4])
    wait_rows(corr, SAME_ROWS, send.at[5])


def in_hbm(x):
    return pltpu.with_memory_space_constraint(x, pltpu.HBM)


def store_kernel(query, key, value, corr, to_query, to_key, to_value, to_filter, flipped, sems):
    copies = [
        pltpu.make_async_copy(*pair, sems.at[i])
        for i, pair in enumerate(((query, to_query), (key, to_key), (value, to_value)))
    ]
    for copy in copies:
        copy.start()
    for i in range(4):
        for j in range(2 * i, 2 * i + 2):
            cols = slice(j * BLOCK, (j + 1) * BLOCK)
            flipped[:, cols] = corr[cols, :].T
        cols = pl.ds(2 * i * BLOCK, 2 * BLOCK)
        copy = pltpu.make_async_copy(flipped.at[:, cols], to_filter.at[:, cols], sems.at[3 + i])
        copy.start()
        copies.append(copy)
    for copy in copies:
        copy.wait()


def shards(query_gate, key_input, value_input, grad_output, filter_raw, skip_gain):
    tab, mid = tables()
    anywhere = pl.BlockSpec(memory_space=pltpu.HBM)
    vmem = pl.BlockSpec(memory_space=pltpu.VMEM)
    signal = pltpu.VMEM((1, BLOCK, WIDTH), BF16)
    narrow = pltpu.VMEM((BLOCK, WIDTH), BF16)
    tall = pltpu.VMEM((WIDTH, BLOCK), F32)
    short = pltpu.VMEM((HALF, BLOCK), F32)
    gain = skip_gain.reshape(1, WIDTH)
    arrays = (query_gate, key_input, value_input, grad_output, filter_raw, gain, tab, mid)
    operands = [in_hbm(x) for x in arrays]
    results = tuple(
        pl.pallas_call(
            kernel,
            out_shape=[signal, signal, signal, pltpu.VMEM((HALF, BLOCK), F32)],
            in_specs=[anywhere] * 8,
            out_specs=[vmem] * 4,
            scratch_shapes=[narrow] * 4
            + [
                pltpu.VMEM((BLOCK, HALF), BF16),
                pltpu.VMEM(tab.shape, BF16),
                pltpu.VMEM(mid.shape, F32),
                pltpu.VMEM((1, WIDTH), F32),
            ]
            + [tall, tall, short] * 3
            + [tall, tall]
            + [
                pltpu.VMEM((OWNED, 2, 2, BLOCK, BLOCK), F32),
                pltpu.VMEM((OWNED, 2, BLOCK, BLOCK), F32),
                pltpu.SemaphoreType.DMA((10,)),
                pltpu.SemaphoreType.DMA((6,)),
                pltpu.SemaphoreType.DMA((6,)),
                pltpu.SemaphoreType.REGULAR((2 * SLAB,)),
            ],
            compiler_params=pltpu.CompilerParams(
                collective_id=0, has_side_effects=True, vmem_limit_bytes=32 * 1024 * 1024
            ),
            name="hyena_back",
        )(*operands)
    )
    return tuple(
        pl.pallas_call(
            store_kernel,
            out_shape=[jax.ShapeDtypeStruct(r.shape, r.dtype) for r in results[:3]]
            + [jax.ShapeDtypeStruct((BLOCK, HALF), F32)],
            in_specs=[vmem] * 4,
            out_specs=[anywhere] * 4,
            scratch_shapes=[
                pltpu.VMEM((BLOCK, HALF), F32),
                pltpu.SemaphoreType.DMA((7,)),
            ],
            compiler_params=pltpu.CompilerParams(vmem_limit_bytes=4 * 1024 * 1024),
            name="store",
        )(*results)
    )


def solution(mesh):
    in_specs = (
        P("ch", "seq", None),
        P("ch", "seq", None),
        P("ch", "seq", None),
        P("ch", "seq", None),
        P("seq", None),
        P(),
    )
    out_specs = (P("ch", "seq", None), P("ch", "seq", None), P("ch", "seq", None), P("seq", "ch"))
    return jax.shard_map(shards, mesh=mesh, in_specs=in_specs, out_specs=out_specs, check_vma=False)
```

```python
import itertools
import math

import jax
import jax.numpy as jnp
import numpy as np
from jax import lax
from jax.experimental import pallas as pl
from jax.experimental.pallas import tpu as pltpu
from jax.sharding import PartitionSpec as P

BLOCK = 128
FULL = 2 * BLOCK * BLOCK
F32 = jnp.float32
BF16 = jnp.bfloat16


def split_table(table):
    high = jnp.asarray(table, F32).astype(BF16)
    low = (jnp.asarray(table, F32) - high.astype(F32)).astype(BF16)
    return (high, low)


def tables():
    idx = np.arange(BLOCK)
    turn_one = 2.0 * math.pi / (2 * BLOCK) * ((idx[:, None] + 0.5) * idx[None, :])
    first = np.concatenate([np.cos(turn_one), -np.sin(turn_one)], axis=0)
    turn_two = 2.0 * math.pi / BLOCK * (idx[:, None] * idx[None, :] % BLOCK)
    cos_two, sin_two = np.cos(turn_two), np.sin(turn_two)
    second = np.block([[cos_two, -sin_two], [sin_two, cos_two]])
    second_inv = np.block([[cos_two, sin_two], [-sin_two, cos_two]])
    turn_mid = 2.0 * math.pi / FULL * ((idx[:, None] + 0.5) * idx[None, :])
    f_high, f_low = split_table(first.astype(np.float32))
    rows = [jnp.concatenate([f_high, f_low], axis=1)]
    for table in (second, second_inv, first.T):
        rows.extend(split_table(table.astype(np.float32)))
    mid = np.concatenate([np.cos(turn_mid), np.sin(turn_mid)], axis=0)
    return (jnp.concatenate(rows, axis=0), jnp.asarray(mid, F32))


def halves(x):
    high = x.astype(BF16)
    return (high, (x - high.astype(F32)).astype(BF16))


def dot(a, b):
    return jnp.dot(a, b, preferred_element_type=F32)


def dot_left(high, low, x):
    x_high, x_low = halves(x)
    return dot(high, x_high) + dot(low, x_high) + dot(high, x_low)


def dot_right(x, high, low):
    x_high, x_low = halves(x)
    return dot(x_high, high) + dot(x_high, low) + dot(x_low, high)


def to_spectrum(parts, tab, mid):
    cos_mid, sin_mid = mid[:BLOCK], mid[BLOCK:]
    lines = dot_left(tab[:256, :BLOCK], tab[:256, BLOCK:], jnp.concatenate(parts, axis=1))
    rows = []
    for i in range(len(parts)):
        re = lines[:BLOCK, i * BLOCK : (i + 1) * BLOCK]
        im = lines[BLOCK:, i * BLOCK : (i + 1) * BLOCK]
        rows.append(
            jnp.concatenate([re * cos_mid + im * sin_mid, im * cos_mid - re * sin_mid], axis=1)
        )
    spec = dot_right(jnp.concatenate(rows, axis=0), tab[256:512], tab[512:768])
    return [
        (spec[i * BLOCK : (i + 1) * BLOCK, :BLOCK], spec[i * BLOCK : (i + 1) * BLOCK, BLOCK:])
        for i in range(len(parts))
    ]


def from_spectrum(specs, tab, mid):
    cos_mid, sin_mid = mid[:BLOCK], mid[BLOCK:]
    rows = jnp.concatenate([jnp.concatenate([re, im], axis=1) for re, im in specs], axis=0)
    grid = dot_right(rows, tab[768:1024], tab[1024:1280])
    cols = []
    for i in range(len(specs)):
        re = grid[i * BLOCK : (i + 1) * BLOCK, :BLOCK]
        im = grid[i * BLOCK : (i + 1) * BLOCK, BLOCK:]
        cols.append(
            jnp.concatenate([re * cos_mid - im * sin_mid, im * cos_mid + re * sin_mid], axis=0)
        )
    lines = dot_left(tab[1280:1408], tab[1408:1536], jnp.concatenate(cols, axis=1))
    return [lines[:, i * BLOCK : (i + 1) * BLOCK] for i in range(len(specs))]


SCALE = 1.0 / (BLOCK * (FULL // 2))
OWNED = 8
WIDTH = 2048
HALF = WIDTH // 2
MESH = pl.DeviceIdType.MESH


def channel_rows(part, channel):
    return pl.ds(part * BLOCK * OWNED + channel, BLOCK, stride=OWNED)


def tile(index):
    return pl.ds(pl.multiple_of(index * OWNED, OWNED), OWNED)


TURNS = (0, 1, 7, 2, 6, 3, 5, 4)
SLAB = BLOCK // 8


def ring_bases(turns=TURNS):
    z = lax.div(lax.axis_index("seq"), SLAB)
    return [lax.rem(z + turn, 8) * SLAB for turn in turns]


def at_step(step):
    place = lax.rem(lax.axis_index("seq"), SLAB) * 2 + lax.axis_index("ch")
    rest = lax.rem(place + step, 2 * SLAB)
    return (lax.div(rest, 2), lax.rem(rest, 2))


def hops_plane(move):
    x, y, core = move
    return (min(x, 4 - x) + min(y, 4 - y), core)


PLANE = sorted(itertools.product(range(4), range(4), range(2)), key=hops_plane)[1:]
NEAR_FIRST = ([move for move in PLANE if move[0] % 2 == 0], [move for move in PLANE if move[0] % 2])


def slab_places(moves):
    seq, ch = lax.axis_index("seq"), lax.axis_index("ch")
    x, y = lax.rem(lax.div(seq, 8), 2) * 2 + ch, lax.rem(lax.div(seq, 2), 4)
    cores = [lax.rem(seq, 2), 1 - lax.rem(seq, 2)]
    xs = [lax.rem(x + i, 4) for i in range(4)]
    highs, lows = [lax.div(i, 2) * 8 for i in xs], [lax.rem(i, 2) for i in xs]
    ys = [lax.rem(y + i, 4) * 2 for i in range(4)]
    return [(highs[dx] + ys[dy] + cores[dcore], lows[dx]) for dx, dy, dcore in moves]


def for_each_peer(visit):
    bases = ring_bases()

    def body(step, carry):
        low, to_ch = at_step(step)
        for base in bases:
            visit(base + low, to_ch)
        return carry

    low, to_ch = at_step(0)
    for base in bases[1:]:
        visit(base + low, to_ch)
    lax.fori_loop(1, 2 * SLAB, body, 0)


def hops(move):
    z, x, y, core = move
    return (2 * x + min(y, 4 - y) + core, min(z, 8 - z))


MOVES = sorted(itertools.product(range(8), range(2), range(4), range(2)), key=hops)[:0:-1]


def hops_all(move):
    z, x, y, core = move
    return (min(x, 4 - x) + min(y, 4 - y) + core, min(z, 8 - z))


MOVES_ALL = sorted(itertools.product(range(8), range(4), range(4), range(2)), key=hops_all)[:0:-1]


def for_each_far(visit):
    seq, ch = lax.axis_index("seq"), lax.axis_index("ch")
    z, x = lax.div(seq, SLAB), lax.rem(lax.div(seq, 8), 2) * 2 + ch
    y, core = lax.rem(lax.div(seq, 2), 4), lax.rem(seq, 2)
    zs = [lax.rem(z + i, 8) * SLAB for i in range(8)]
    xs = [lax.rem(x + i, 4) for i in range(4)]
    highs, lows = [lax.div(i, 2) * 8 for i in xs], [lax.rem(i, 2) for i in xs]
    ys = [lax.rem(y + i, 4) * 2 for i in range(4)]
    cores = [core, 1 - core]
    for move in MOVES_ALL:
        visit(zs[move[0]] + highs[move[1]] + ys[move[2]] + cores[move[3]], lows[move[1]])


def for_each_same(visit):
    seq = lax.axis_index("seq")
    z, x = lax.div(seq, SLAB), lax.rem(lax.div(seq, 8), 2)
    y, core = lax.rem(lax.div(seq, 2), 4), lax.rem(seq, 2)
    zs = [lax.rem(z + i, 8) * SLAB for i in range(8)]
    xs = [lax.rem(x + i, 2) * 8 for i in range(2)]
    ys = [lax.rem(y + i, 4) * 2 for i in range(4)]
    cores = [core, 1 - core]
    for move in MOVES:
        visit(zs[move[0]] + xs[move[1]] + ys[move[2]] + cores[move[3]])


def tile_sender(source, target, send, recv):
    me = lax.axis_index("ch") * BLOCK + lax.axis_index("seq")

    def visit(to_seq, to_ch):
        pltpu.make_async_remote_copy(
            src_ref=source.at[tile(to_ch * BLOCK + to_seq)],
            dst_ref=target.at[tile(me)],
            send_sem=send,
            recv_sem=recv,
            device_id=(to_seq, to_ch),
            device_id_type=MESH,
        ).start()

    return visit


def keep_own(source, target):
    me = lax.axis_index("ch") * BLOCK + lax.axis_index("seq")
    target[tile(me), :] = source[tile(me), :]


def send_all(source, target, send, recv, visits=None):
    (visits or for_each_peer)(tile_sender(source, target, send, recv))
    keep_own(source, target)


def send_same(source, target, send, recv):
    seq, ch = lax.axis_index("seq"), lax.axis_index("ch")

    def visit(to_seq):
        pltpu.make_async_remote_copy(
            src_ref=source.at[tile(to_seq)],
            dst_ref=target.at[tile(seq)],
            send_sem=send,
            recv_sem=recv,
            device_id=(to_seq, ch),
            device_id_type=MESH,
        ).start()

    for_each_same(visit)
    target[tile(seq), :] = source[tile(seq), :]


def wait_rows(ref, rows, sem):
    part = ref.at[pl.ds(0, rows)]
    pltpu.make_async_copy(part, part, sem).wait()


ALL_ROWS = WIDTH - OWNED
SAME_ROWS = HALF - OWNED


def kernel(
    query_hbm,
    key_hbm,
    value_hbm,
    out_hbm,
    filter_hbm,
    gain_hbm,
    tab_hbm,
    mid_hbm,
    grad_query,
    grad_key,
    grad_value,
    corr_in,
    query,
    key,
    value,
    out,
    taps,
    tab_ref,
    mid_ref,
    gain_ref,
    mixed_t,
    gated_t,
    taps_t,
    mixed_in,
    gated_in,
    taps_in,
    conv,
    back,
    corr,
    conv_in,
    back_in,
    mspec,
    tspec,
    load,
    send,
    recv,
    ready,
):
    seq, ch = lax.axis_index("seq"), lax.axis_index("ch")
    barrier = pltpu.get_barrier_semaphore()

    def own_half(ref):
        return ref.at[:, pl.ds(pl.multiple_of(ch * HALF, HALF), HALF)]

    def other_half(ref):
        return ref.at[:, pl.ds(pl.multiple_of((1 - ch) * HALF, HALF), HALF)]

    key_src, value_src = key_hbm.at[0], value_hbm.at[0]
    loads = [
        pltpu.make_async_copy(own_half(key_src), own_half(key), load.at[0]),
        pltpu.make_async_copy(own_half(value_src), own_half(value), load.at[1]),
        pltpu.make_async_copy(other_half(key_src), other_half(key), load.at[2]),
        pltpu.make_async_copy(other_half(value_src), other_half(value), load.at[3]),
        pltpu.make_async_copy(own_half(filter_hbm), taps, load.at[4]),
        pltpu.make_async_copy(out_hbm.at[0], out, load.at[5]),
        pltpu.make_async_copy(query_hbm.at[0], query, load.at[6]),
        pltpu.make_async_copy(tab_hbm, tab_ref, load.at[7]),
        pltpu.make_async_copy(mid_hbm, mid_ref, load.at[8]),
        pltpu.make_async_copy(gain_hbm, gain_ref, load.at[9]),
    ]
    for copy in loads[:4]:
        copy.start()

    bases = ring_bases()

    def greet(to_seq, to_ch):
        pl.semaphore_signal(barrier, inc=1, device_id=(to_seq, to_ch), device_id_type=MESH)

    with jax.named_scope("greet"):
        for base in bases[:0:-1]:
            greet(base + lax.rem(seq, SLAB), ch)
        for low, to_ch in slab_places(PLANE[::-1]):
            greet(bases[0] + low, to_ch)
        for copy in loads[4:]:
            copy.start()

    def flip_product(left, right, target, first=0, count=WIDTH // BLOCK):
        def body(j, carry):
            cols = pl.ds(pl.multiple_of(first + j * BLOCK, BLOCK), BLOCK)
            target[cols, :] = (left[:, cols].astype(F32) * right[:, cols].astype(F32)).T
            return carry

        lax.fori_loop(0, count, body, 0)

    def flip_taps(j, carry):
        cols = pl.ds(pl.multiple_of(j * BLOCK, BLOCK), BLOCK)
        taps_t[cols, :] = taps[:, cols].astype(F32).T
        return carry

    send_mixed = tile_sender(mixed_t, mixed_in, send.at[0], recv.at[0])

    def mixed_steps(moves):
        for low, to_ch in slab_places(moves):
            pl.semaphore_wait(ready.at[2 * low + to_ch], 1)
            for base in bases:
                send_mixed(base + low, to_ch)

    with jax.named_scope("barrier"):
        pl.semaphore_wait(barrier, 7 + 2 * SLAB - 1)
        mine = ready.at[2 * lax.rem(seq, SLAB) + ch]
        for low, to_ch in slab_places(PLANE[::-1]):
            pl.semaphore_signal(
                mine, inc=1, device_id=(bases[0] + low, to_ch), device_id_type=MESH
            )
    with jax.named_scope("load"):
        loads[0].wait()
        loads[1].wait()
    with jax.named_scope("flip_mixed"):
        flip_product(key, value, mixed_t, ch * HALF, HALF // BLOCK)
    with jax.named_scope("send_mixed"):
        for base in bases[1:]:
            send_mixed(base + lax.rem(seq, SLAB), ch)
        mixed_steps(NEAR_FIRST[0])
    with jax.named_scope("flip_mixed2"):
        loads[2].wait()
        loads[3].wait()
        flip_product(key, value, mixed_t, (1 - ch) * HALF, HALF // BLOCK)
    with jax.named_scope("send_mixed2"):
        mixed_steps(NEAR_FIRST[1])
        keep_own(mixed_t, mixed_in)
    with jax.named_scope("flip_taps"):
        loads[4].wait()
        lax.fori_loop(0, HALF // BLOCK, flip_taps, 0)
    with jax.named_scope("send_taps"):
        send_same(taps_t, taps_in, send.at[1], recv.at[1])
    loads[5].wait()
    loads[6].wait()
    with jax.named_scope("flip_gated"):
        flip_product(out, query, gated_t)
    with jax.named_scope("send_gated"):
        send_all(gated_t, gated_in, send.at[2], recv.at[2], for_each_far)
    for copy in loads[7:]:
        copy.wait()
    with jax.named_scope("wait_mixed"):
        wait_rows(mixed_in, ALL_ROWS, recv.at[0])
        wait_rows(taps_in, SAME_ROWS, recv.at[1])

    def conv_body(c, carry):
        tab, mid = tab_ref[...], mid_ref[...]
        parts = [mixed_in[channel_rows(b, c), :] for b in range(2)]
        parts.append(taps_in[channel_rows(0, c), :])
        mixed_a, mixed_b, taps_spec = to_spectrum(parts, tab, mid)
        t_re, t_im = taps_spec
        prods = []
        for b, (re, im) in enumerate((mixed_a, mixed_b)):
            mspec[c, b, 0] = re
            mspec[c, b, 1] = im
            prods.append((re * t_re - im * t_im, re * t_im + im * t_re))
        tspec[c, 0] = t_re
        tspec[c, 1] = t_im
        lines = from_spectrum(prods, tab, mid)
        for b in range(2):
            conv[channel_rows(b, c), :] = lines[b] * SCALE
        return carry

    with jax.named_scope("conv"):
        lax.fori_loop(0, OWNED, conv_body, 0)
    with jax.named_scope("send_conv"):
        send_all(conv, conv_in, send.at[3], recv.at[3], for_each_far)
    with jax.named_scope("wait_gated"):
        wait_rows(gated_in, ALL_ROWS, recv.at[2])

    def back_body(c, carry):
        tab, mid = tab_ref[...], mid_ref[...]
        gated = to_spectrum([gated_in[channel_rows(b, c), :] for b in range(2)], tab, mid)
        t_re, t_im = tspec[c, 0], tspec[c, 1]
        prods = []
        terms = []
        for b, (re, im) in enumerate(gated):
            m_re, m_im = mspec[c, b, 0], mspec[c, b, 1]
            prods.append((t_re * re + t_im * im, t_re * im - t_im * re))
            terms.append((m_re * re + m_im * im, m_re * im - m_im * re))
        prods.append((terms[0][0] + terms[1][0], terms[0][1] + terms[1][1]))
        lines = from_spectrum(prods, tab, mid)
        for b in range(2):
            back[channel_rows(b, c), :] = lines[b] * SCALE
        corr[channel_rows(0, c), :] = lines[2] * SCALE
        return carry

    with jax.named_scope("back"):
        lax.fori_loop(0, OWNED, back_body, 0)
    with jax.named_scope("send_back"):
        send_all(back, back_in, send.at[4], recv.at[4], for_each_far)
        send_same(corr, corr_in, send.at[5], recv.at[5])

    with jax.named_scope("wait_conv"):
        wait_rows(conv_in, ALL_ROWS, recv.at[3])

    def query_body(j, carry):
        cols = pl.ds(pl.multiple_of(j * BLOCK, BLOCK), BLOCK)
        mixed = key[:, cols].astype(F32) * value[:, cols].astype(F32)
        full = conv_in[cols, :].T + gain_ref[:, cols] * mixed
        grad_query[0, :, cols] = (out[:, cols].astype(F32) * full).astype(BF16)
        return carry

    with jax.named_scope("query_out"):
        lax.fori_loop(0, WIDTH // BLOCK, query_body, 0)
    with jax.named_scope("wait_back"):
        wait_rows(back_in, ALL_ROWS, recv.at[4])

    def back_out(j, carry):
        cols = pl.ds(pl.multiple_of(j * BLOCK, BLOCK), BLOCK)
        gated = out[:, cols].astype(F32) * query[:, cols].astype(F32)
        full = back_in[cols, :].T + gain_ref[:, cols] * gated
        grad_key[0, :, cols] = (full * value[:, cols].astype(F32)).astype(BF16)
        grad_value[0, :, cols] = (full * key[:, cols].astype(F32)).astype(BF16)
        return carry

    with jax.named_scope("back_out"):
        lax.fori_loop(0, WIDTH // BLOCK, back_out, 0)
    with jax.named_scope("wait_corr"):
        wait_rows(corr_in, SAME_ROWS, recv.at[5])
    wait_rows(mixed_t, ALL_ROWS, send.at[0])
    wait_rows(taps_t, SAME_ROWS, send.at[1])
    wait_rows(gated_t, ALL_ROWS, send.at[2])
    wait_rows(conv, ALL_ROWS, send.at[3])
    wait_rows(back, ALL_ROWS, send.at[4])
    wait_rows(corr, SAME_ROWS, send.at[5])


def in_hbm(x):
    return pltpu.with_memory_space_constraint(x, pltpu.HBM)


def store_kernel(query, key, value, corr, to_query, to_key, to_value, to_filter, flipped, sems):
    copies = [
        pltpu.make_async_copy(*pair, sems.at[i])
        for i, pair in enumerate(((query, to_query), (key, to_key), (value, to_value)))
    ]
    for copy in copies:
        copy.start()
    for i in range(4):
        for j in range(2 * i, 2 * i + 2):
            cols = slice(j * BLOCK, (j + 1) * BLOCK)
            flipped[:, cols] = corr[cols, :].T
        cols = pl.ds(2 * i * BLOCK, 2 * BLOCK)
        copy = pltpu.make_async_copy(flipped.at[:, cols], to_filter.at[:, cols], sems.at[3 + i])
        copy.start()
        copies.append(copy)
    for copy in copies:
        copy.wait()


def shards(query_gate, key_input, value_input, grad_output, filter_raw, skip_gain):
    tab, mid = tables()
    anywhere = pl.BlockSpec(memory_space=pltpu.HBM)
    vmem = pl.BlockSpec(memory_space=pltpu.VMEM)
    signal = pltpu.VMEM((1, BLOCK, WIDTH), BF16)
    narrow = pltpu.VMEM((BLOCK, WIDTH), BF16)
    tall = pltpu.VMEM((WIDTH, BLOCK), F32)
    short = pltpu.VMEM((HALF, BLOCK), F32)
    gain = skip_gain.reshape(1, WIDTH)
    arrays = (query_gate, key_input, value_input, grad_output, filter_raw, gain, tab, mid)
    operands = [in_hbm(x) for x in arrays]
    results = tuple(
        pl.pallas_call(
            kernel,
            out_shape=[signal, signal, signal, pltpu.VMEM((HALF, BLOCK), F32)],
            in_specs=[anywhere] * 8,
            out_specs=[vmem] * 4,
            scratch_shapes=[narrow] * 4
            + [
                pltpu.VMEM((BLOCK, HALF), BF16),
                pltpu.VMEM(tab.shape, BF16),
                pltpu.VMEM(mid.shape, F32),
                pltpu.VMEM((1, WIDTH), F32),
            ]
            + [tall, tall, short] * 3
            + [tall, tall]
            + [
                pltpu.VMEM((OWNED, 2, 2, BLOCK, BLOCK), F32),
                pltpu.VMEM((OWNED, 2, BLOCK, BLOCK), F32),
                pltpu.SemaphoreType.DMA((10,)),
                pltpu.SemaphoreType.DMA((6,)),
                pltpu.SemaphoreType.DMA((6,)),
                pltpu.SemaphoreType.REGULAR((2 * SLAB,)),
            ],
            compiler_params=pltpu.CompilerParams(
                collective_id=0, has_side_effects=True, vmem_limit_bytes=32 * 1024 * 1024
            ),
            name="hyena_back",
        )(*operands)
    )
    return tuple(
        pl.pallas_call(
            store_kernel,
            out_shape=[jax.ShapeDtypeStruct(r.shape, r.dtype) for r in results[:3]]
            + [jax.ShapeDtypeStruct((BLOCK, HALF), F32)],
            in_specs=[vmem] * 4,
            out_specs=[anywhere] * 4,
            scratch_shapes=[
                pltpu.VMEM((BLOCK, HALF), F32),
                pltpu.SemaphoreType.DMA((7,)),
            ],
            compiler_params=pltpu.CompilerParams(vmem_limit_bytes=4 * 1024 * 1024),
            name="store",
        )(*results)
    )


def solution(mesh):
    in_specs = (
        P("ch", "seq", None),
        P("ch", "seq", None),
        P("ch", "seq", None),
        P("ch", "seq", None),
        P("seq", None),
        P(),
    )
    out_specs = (P("ch", "seq", None), P("ch", "seq", None), P("ch", "seq", None), P("seq", "ch"))
    return jax.shard_map(shards, mesh=mesh, in_specs=in_specs, out_specs=out_specs, check_vma=False)
```

```python
import itertools
import math

import jax
import jax.numpy as jnp
import numpy as np
from jax import lax
from jax.experimental import pallas as pl
from jax.experimental.pallas import tpu as pltpu
from jax.sharding import PartitionSpec as P

BLOCK = 128
FULL = 2 * BLOCK * BLOCK
F32 = jnp.float32
BF16 = jnp.bfloat16


def split_table(table):
    high = jnp.asarray(table, F32).astype(BF16)
    low = (jnp.asarray(table, F32) - high.astype(F32)).astype(BF16)
    return (high, low)


def tables():
    idx = np.arange(BLOCK)
    turn_one = 2.0 * math.pi / (2 * BLOCK) * ((idx[:, None] + 0.5) * idx[None, :])
    first = np.concatenate([np.cos(turn_one), -np.sin(turn_one)], axis=0)
    turn_two = 2.0 * math.pi / BLOCK * (idx[:, None] * idx[None, :] % BLOCK)
    cos_two, sin_two = np.cos(turn_two), np.sin(turn_two)
    second = np.block([[cos_two, -sin_two], [sin_two, cos_two]])
    second_inv = np.block([[cos_two, sin_two], [-sin_two, cos_two]])
    turn_mid = 2.0 * math.pi / FULL * ((idx[:, None] + 0.5) * idx[None, :])
    f_high, f_low = split_table(first.astype(np.float32))
    rows = [jnp.concatenate([f_high, f_low], axis=1)]
    for table in (second, second_inv, first.T):
        rows.extend(split_table(table.astype(np.float32)))
    mid = np.concatenate([np.cos(turn_mid), np.sin(turn_mid)], axis=0)
    return (jnp.concatenate(rows, axis=0), jnp.asarray(mid, F32))


def halves(x):
    high = x.astype(BF16)
    return (high, (x - high.astype(F32)).astype(BF16))


def dot(a, b):
    return jnp.dot(a, b, preferred_element_type=F32)


def dot_left(high, low, x):
    x_high, x_low = halves(x)
    return dot(high, x_high) + dot(low, x_high) + dot(high, x_low)


def dot_right(x, high, low):
    x_high, x_low = halves(x)
    return dot(x_high, high) + dot(x_high, low) + dot(x_low, high)


def to_spectrum(parts, tab, mid):
    cos_mid, sin_mid = mid[:BLOCK], mid[BLOCK:]
    lines = dot_left(tab[:256, :BLOCK], tab[:256, BLOCK:], jnp.concatenate(parts, axis=1))
    rows = []
    for i in range(len(parts)):
        re = lines[:BLOCK, i * BLOCK : (i + 1) * BLOCK]
        im = lines[BLOCK:, i * BLOCK : (i + 1) * BLOCK]
        rows.append(
            jnp.concatenate([re * cos_mid + im * sin_mid, im * cos_mid - re * sin_mid], axis=1)
        )
    spec = dot_right(jnp.concatenate(rows, axis=0), tab[256:512], tab[512:768])
    return [
        (spec[i * BLOCK : (i + 1) * BLOCK, :BLOCK], spec[i * BLOCK : (i + 1) * BLOCK, BLOCK:])
        for i in range(len(parts))
    ]


def from_spectrum(specs, tab, mid):
    cos_mid, sin_mid = mid[:BLOCK], mid[BLOCK:]
    rows = jnp.concatenate([jnp.concatenate([re, im], axis=1) for re, im in specs], axis=0)
    grid = dot_right(rows, tab[768:1024], tab[1024:1280])
    cols = []
    for i in range(len(specs)):
        re = grid[i * BLOCK : (i + 1) * BLOCK, :BLOCK]
        im = grid[i * BLOCK : (i + 1) * BLOCK, BLOCK:]
        cols.append(
            jnp.concatenate([re * cos_mid - im * sin_mid, im * cos_mid + re * sin_mid], axis=0)
        )
    lines = dot_left(tab[1280:1408], tab[1408:1536], jnp.concatenate(cols, axis=1))
    return [lines[:, i * BLOCK : (i + 1) * BLOCK] for i in range(len(specs))]


SCALE = 1.0 / (BLOCK * (FULL // 2))
OWNED = 8
WIDTH = 2048
HALF = WIDTH // 2
MESH = pl.DeviceIdType.MESH


def channel_rows(part, channel):
    return pl.ds(part * BLOCK * OWNED + channel, BLOCK, stride=OWNED)


def tile(index):
    return pl.ds(pl.multiple_of(index * OWNED, OWNED), OWNED)


TURNS = (0, 1, 7, 2, 6, 3, 5, 4)
SLAB = BLOCK // 8


def ring_bases(turns=TURNS):
    z = lax.div(lax.axis_index("seq"), SLAB)
    return [lax.rem(z + turn, 8) * SLAB for turn in turns]


def at_step(step):
    place = lax.rem(lax.axis_index("seq"), SLAB) * 2 + lax.axis_index("ch")
    rest = lax.rem(place + step, 2 * SLAB)
    return (lax.div(rest, 2), lax.rem(rest, 2))


def hops_plane(move):
    x, y, core = move
    return (min(x, 4 - x) + min(y, 4 - y), core)


PLANE = sorted(itertools.product(range(4), range(4), range(2)), key=hops_plane)[1:]
NEAR_FIRST = ([move for move in PLANE if move[0] % 2 == 0], [move for move in PLANE if move[0] % 2])


def slab_places(moves):
    seq, ch = lax.axis_index("seq"), lax.axis_index("ch")
    x, y = lax.rem(lax.div(seq, 8), 2) * 2 + ch, lax.rem(lax.div(seq, 2), 4)
    cores = [lax.rem(seq, 2), 1 - lax.rem(seq, 2)]
    xs = [lax.rem(x + i, 4) for i in range(4)]
    highs, lows = [lax.div(i, 2) * 8 for i in xs], [lax.rem(i, 2) for i in xs]
    ys = [lax.rem(y + i, 4) * 2 for i in range(4)]
    return [(highs[dx] + ys[dy] + cores[dcore], lows[dx]) for dx, dy, dcore in moves]


def for_each_peer(visit):
    bases = ring_bases()

    def body(step, carry):
        low, to_ch = at_step(step)
        for base in bases:
            visit(base + low, to_ch)
        return carry

    low, to_ch = at_step(0)
    for base in bases[1:]:
        visit(base + low, to_ch)
    lax.fori_loop(1, 2 * SLAB, body, 0)


def hops(move):
    z, x, y, core = move
    return (2 * x + min(y, 4 - y) + 1 - core, min(z, 8 - z))


MOVES = sorted(itertools.product(range(8), range(2), range(4), range(2)), key=hops)[::-1]
MOVES = [move for move in MOVES if any(move[:3])]


def hops_all(move):
    z, x, y, core = move
    return (min(x, 4 - x) + min(y, 4 - y) + 1 - core, min(z, 8 - z))


MOVES_ALL = sorted(itertools.product(range(8), range(4), range(4), range(2)), key=hops_all)[::-1]
MOVES_ALL = [move for move in MOVES_ALL if any(move[:3])]


def for_each_far(visit):
    seq, ch = lax.axis_index("seq"), lax.axis_index("ch")
    z, x = lax.div(seq, SLAB), lax.rem(lax.div(seq, 8), 2) * 2 + ch
    y, core = lax.rem(lax.div(seq, 2), 4), lax.rem(seq, 2)
    zs = [lax.rem(z + i, 8) * SLAB for i in range(8)]
    xs = [lax.rem(x + i, 4) for i in range(4)]
    highs, lows = [lax.div(i, 2) * 8 for i in xs], [lax.rem(i, 2) for i in xs]
    ys = [lax.rem(y + i, 4) * 2 for i in range(4)]
    for move in MOVES_ALL:
        visit(zs[move[0]] + highs[move[1]] + ys[move[2]] + move[3], lows[move[1]])
    visit(zs[0] + highs[0] + ys[0] + 1 - core, lows[0])


def for_each_same(visit):
    seq = lax.axis_index("seq")
    z, x = lax.div(seq, SLAB), lax.rem(lax.div(seq, 8), 2)
    y, core = lax.rem(lax.div(seq, 2), 4), lax.rem(seq, 2)
    zs = [lax.rem(z + i, 8) * SLAB for i in range(8)]
    xs = [lax.rem(x + i, 2) * 8 for i in range(2)]
    ys = [lax.rem(y + i, 4) * 2 for i in range(4)]
    for move in MOVES:
        visit(zs[move[0]] + xs[move[1]] + ys[move[2]] + move[3])
    visit(zs[0] + xs[0] + ys[0] + 1 - core)


def tile_sender(source, target, send, recv):
    me = lax.axis_index("ch") * BLOCK + lax.axis_index("seq")

    def visit(to_seq, to_ch):
        pltpu.make_async_remote_copy(
            src_ref=source.at[tile(to_ch * BLOCK + to_seq)],
            dst_ref=target.at[tile(me)],
            send_sem=send,
            recv_sem=recv,
            device_id=(to_seq, to_ch),
            device_id_type=MESH,
        ).start()

    return visit


def keep_own(source, target):
    me = lax.axis_index("ch") * BLOCK + lax.axis_index("seq")
    target[tile(me), :] = source[tile(me), :]


def send_all(source, target, send, recv, visits=None):
    (visits or for_each_peer)(tile_sender(source, target, send, recv))
    keep_own(source, target)


def send_same(source, target, send, recv):
    seq, ch = lax.axis_index("seq"), lax.axis_index("ch")

    def visit(to_seq):
        pltpu.make_async_remote_copy(
            src_ref=source.at[tile(to_seq)],
            dst_ref=target.at[tile(seq)],
            send_sem=send,
            recv_sem=recv,
            device_id=(to_seq, ch),
            device_id_type=MESH,
        ).start()

    for_each_same(visit)
    target[tile(seq), :] = source[tile(seq), :]


def wait_rows(ref, rows, sem):
    part = ref.at[pl.ds(0, rows)]
    pltpu.make_async_copy(part, part, sem).wait()


ALL_ROWS = WIDTH - OWNED
SAME_ROWS = HALF - OWNED


def kernel(
    query_hbm,
    key_hbm,
    value_hbm,
    out_hbm,
    filter_hbm,
    gain_hbm,
    tab_hbm,
    mid_hbm,
    grad_query,
    grad_key,
    grad_value,
    corr_in,
    query,
    key,
    value,
    out,
    taps,
    tab_ref,
    mid_ref,
    gain_ref,
    mixed_t,
    gated_t,
    taps_t,
    mixed_in,
    gated_in,
    taps_in,
    conv,
    back,
    corr,
    conv_in,
    back_in,
    mspec,
    tspec,
    load,
    send,
    recv,
    ready,
):
    seq, ch = lax.axis_index("seq"), lax.axis_index("ch")
    barrier = pltpu.get_barrier_semaphore()

    def own_half(ref):
        return ref.at[:, pl.ds(pl.multiple_of(ch * HALF, HALF), HALF)]

    def other_half(ref):
        return ref.at[:, pl.ds(pl.multiple_of((1 - ch) * HALF, HALF), HALF)]

    key_src, value_src = key_hbm.at[0], value_hbm.at[0]
    loads = [
        pltpu.make_async_copy(own_half(key_src), own_half(key), load.at[0]),
        pltpu.make_async_copy(own_half(value_src), own_half(value), load.at[1]),
        pltpu.make_async_copy(other_half(key_src), other_half(key), load.at[2]),
        pltpu.make_async_copy(other_half(value_src), other_half(value), load.at[3]),
        pltpu.make_async_copy(own_half(filter_hbm), taps, load.at[4]),
        pltpu.make_async_copy(out_hbm.at[0], out, load.at[5]),
        pltpu.make_async_copy(query_hbm.at[0], query, load.at[6]),
        pltpu.make_async_copy(tab_hbm, tab_ref, load.at[7]),
        pltpu.make_async_copy(mid_hbm, mid_ref, load.at[8]),
        pltpu.make_async_copy(gain_hbm, gain_ref, load.at[9]),
    ]
    for copy in loads[:4]:
        copy.start()

    bases = ring_bases()

    def greet(to_seq, to_ch):
        pl.semaphore_signal(barrier, inc=1, device_id=(to_seq, to_ch), device_id_type=MESH)

    with jax.named_scope("greet"):
        for base in bases[:0:-1]:
            greet(base + lax.rem(seq, SLAB), ch)
        for low, to_ch in slab_places(PLANE[::-1]):
            greet(bases[0] + low, to_ch)
        for copy in loads[4:]:
            copy.start()

    def flip_product(left, right, target, first=0, count=WIDTH // BLOCK):
        def body(j, carry):
            cols = pl.ds(pl.multiple_of(first + j * BLOCK, BLOCK), BLOCK)
            target[cols, :] = (left[:, cols].astype(F32) * right[:, cols].astype(F32)).T
            return carry

        lax.fori_loop(0, count, body, 0)

    def flip_taps(j, carry):
        cols = pl.ds(pl.multiple_of(j * BLOCK, BLOCK), BLOCK)
        taps_t[cols, :] = taps[:, cols].astype(F32).T
        return carry

    send_mixed = tile_sender(mixed_t, mixed_in, send.at[0], recv.at[0])

    def mixed_steps(moves):
        for low, to_ch in slab_places(moves):
            pl.semaphore_wait(ready.at[2 * low + to_ch], 1)
            for base in bases:
                send_mixed(base + low, to_ch)

    with jax.named_scope("barrier"):
        pl.semaphore_wait(barrier, 7 + 2 * SLAB - 1)
        mine = ready.at[2 * lax.rem(seq, SLAB) + ch]
        for low, to_ch in slab_places(PLANE[::-1]):
            pl.semaphore_signal(
                mine, inc=1, device_id=(bases[0] + low, to_ch), device_id_type=MESH
            )
    with jax.named_scope("load"):
        loads[0].wait()
        loads[1].wait()
    with jax.named_scope("flip_mixed"):
        flip_product(key, value, mixed_t, ch * HALF, HALF // BLOCK)
    with jax.named_scope("send_mixed"):
        for base in bases[1:]:
            send_mixed(base + lax.rem(seq, SLAB), ch)
        mixed_steps(NEAR_FIRST[0])
    with jax.named_scope("flip_mixed2"):
        loads[2].wait()
        loads[3].wait()
        flip_product(key, value, mixed_t, (1 - ch) * HALF, HALF // BLOCK)
    with jax.named_scope("send_mixed2"):
        mixed_steps(NEAR_FIRST[1])
        keep_own(mixed_t, mixed_in)
    with jax.named_scope("flip_taps"):
        loads[4].wait()
        lax.fori_loop(0, HALF // BLOCK, flip_taps, 0)
    with jax.named_scope("send_taps"):
        send_same(taps_t, taps_in, send.at[1], recv.at[1])
    loads[5].wait()
    loads[6].wait()
    with jax.named_scope("flip_gated"):
        flip_product(out, query, gated_t)
    with jax.named_scope("send_gated"):
        send_all(gated_t, gated_in, send.at[2], recv.at[2], for_each_far)
    for copy in loads[7:]:
        copy.wait()
    with jax.named_scope("wait_mixed"):
        wait_rows(mixed_in, ALL_ROWS, recv.at[0])
        wait_rows(taps_in, SAME_ROWS, recv.at[1])

    def conv_body(c, carry):
        tab, mid = tab_ref[...], mid_ref[...]
        parts = [mixed_in[channel_rows(b, c), :] for b in range(2)]
        parts.append(taps_in[channel_rows(0, c), :])
        mixed_a, mixed_b, taps_spec = to_spectrum(parts, tab, mid)
        t_re, t_im = taps_spec
        prods = []
        for b, (re, im) in enumerate((mixed_a, mixed_b)):
            mspec[c, b, 0] = re
            mspec[c, b, 1] = im
            prods.append((re * t_re - im * t_im, re * t_im + im * t_re))
        tspec[c, 0] = t_re
        tspec[c, 1] = t_im
        lines = from_spectrum(prods, tab, mid)
        for b in range(2):
            conv[channel_rows(b, c), :] = lines[b] * SCALE
        return carry

    with jax.named_scope("conv"):
        lax.fori_loop(0, OWNED, conv_body, 0)
    with jax.named_scope("send_conv"):
        send_all(conv, conv_in, send.at[3], recv.at[3], for_each_far)
    with jax.named_scope("wait_gated"):
        wait_rows(gated_in, ALL_ROWS, recv.at[2])

    def back_body(c, carry):
        tab, mid = tab_ref[...], mid_ref[...]
        gated = to_spectrum([gated_in[channel_rows(b, c), :] for b in range(2)], tab, mid)
        t_re, t_im = tspec[c, 0], tspec[c, 1]
        prods = []
        terms = []
        for b, (re, im) in enumerate(gated):
            m_re, m_im = mspec[c, b, 0], mspec[c, b, 1]
            prods.append((t_re * re + t_im * im, t_re * im - t_im * re))
            terms.append((m_re * re + m_im * im, m_re * im - m_im * re))
        prods.append((terms[0][0] + terms[1][0], terms[0][1] + terms[1][1]))
        lines = from_spectrum(prods, tab, mid)
        for b in range(2):
            back[channel_rows(b, c), :] = lines[b] * SCALE
        corr[channel_rows(0, c), :] = lines[2] * SCALE
        return carry

    with jax.named_scope("back"):
        lax.fori_loop(0, OWNED, back_body, 0)
    with jax.named_scope("send_back"):
        send_all(back, back_in, send.at[4], recv.at[4], for_each_far)
        send_same(corr, corr_in, send.at[5], recv.at[5])

    with jax.named_scope("wait_conv"):
        wait_rows(conv_in, ALL_ROWS, recv.at[3])

    def query_body(j, carry):
        cols = pl.ds(pl.multiple_of(j * BLOCK, BLOCK), BLOCK)
        mixed = key[:, cols].astype(F32) * value[:, cols].astype(F32)
        full = conv_in[cols, :].T + gain_ref[:, cols] * mixed
        grad_query[0, :, cols] = (out[:, cols].astype(F32) * full).astype(BF16)
        return carry

    with jax.named_scope("query_out"):
        lax.fori_loop(0, WIDTH // BLOCK, query_body, 0)
    with jax.named_scope("wait_back"):
        wait_rows(back_in, ALL_ROWS, recv.at[4])

    def back_out(j, carry):
        cols = pl.ds(pl.multiple_of(j * BLOCK, BLOCK), BLOCK)
        gated = out[:, cols].astype(F32) * query[:, cols].astype(F32)
        full = back_in[cols, :].T + gain_ref[:, cols] * gated
        grad_key[0, :, cols] = (full * value[:, cols].astype(F32)).astype(BF16)
        grad_value[0, :, cols] = (full * key[:, cols].astype(F32)).astype(BF16)
        return carry

    with jax.named_scope("back_out"):
        lax.fori_loop(0, WIDTH // BLOCK, back_out, 0)
    with jax.named_scope("wait_corr"):
        wait_rows(corr_in, SAME_ROWS, recv.at[5])
    wait_rows(mixed_t, ALL_ROWS, send.at[0])
    wait_rows(taps_t, SAME_ROWS, send.at[1])
    wait_rows(gated_t, ALL_ROWS, send.at[2])
    wait_rows(conv, ALL_ROWS, send.at[3])
    wait_rows(back, ALL_ROWS, send.at[4])
    wait_rows(corr, SAME_ROWS, send.at[5])


def in_hbm(x):
    return pltpu.with_memory_space_constraint(x, pltpu.HBM)


def store_kernel(query, key, value, corr, to_query, to_key, to_value, to_filter, flipped, sems):
    copies = [
        pltpu.make_async_copy(*pair, sems.at[i])
        for i, pair in enumerate(((query, to_query), (key, to_key), (value, to_value)))
    ]
    for copy in copies:
        copy.start()
    for i in range(4):
        for j in range(2 * i, 2 * i + 2):
            cols = slice(j * BLOCK, (j + 1) * BLOCK)
            flipped[:, cols] = corr[cols, :].T
        cols = pl.ds(2 * i * BLOCK, 2 * BLOCK)
        copy = pltpu.make_async_copy(flipped.at[:, cols], to_filter.at[:, cols], sems.at[3 + i])
        copy.start()
        copies.append(copy)
    for copy in copies:
        copy.wait()


def shards(query_gate, key_input, value_input, grad_output, filter_raw, skip_gain):
    tab, mid = tables()
    anywhere = pl.BlockSpec(memory_space=pltpu.HBM)
    vmem = pl.BlockSpec(memory_space=pltpu.VMEM)
    signal = pltpu.VMEM((1, BLOCK, WIDTH), BF16)
    narrow = pltpu.VMEM((BLOCK, WIDTH), BF16)
    tall = pltpu.VMEM((WIDTH, BLOCK), F32)
    short = pltpu.VMEM((HALF, BLOCK), F32)
    gain = skip_gain.reshape(1, WIDTH)
    arrays = (query_gate, key_input, value_input, grad_output, filter_raw, gain, tab, mid)
    operands = [in_hbm(x) for x in arrays]
    results = tuple(
        pl.pallas_call(
            kernel,
            out_shape=[signal, signal, signal, pltpu.VMEM((HALF, BLOCK), F32)],
            in_specs=[anywhere] * 8,
            out_specs=[vmem] * 4,
            scratch_shapes=[narrow] * 4
            + [
                pltpu.VMEM((BLOCK, HALF), BF16),
                pltpu.VMEM(tab.shape, BF16),
                pltpu.VMEM(mid.shape, F32),
                pltpu.VMEM((1, WIDTH), F32),
            ]
            + [tall, tall, short] * 3
            + [tall, tall]
            + [
                pltpu.VMEM((OWNED, 2, 2, BLOCK, BLOCK), F32),
                pltpu.VMEM((OWNED, 2, BLOCK, BLOCK), F32),
                pltpu.SemaphoreType.DMA((10,)),
                pltpu.SemaphoreType.DMA((6,)),
                pltpu.SemaphoreType.DMA((6,)),
                pltpu.SemaphoreType.REGULAR((2 * SLAB,)),
            ],
            compiler_params=pltpu.CompilerParams(
                collective_id=0, has_side_effects=True, vmem_limit_bytes=32 * 1024 * 1024
            ),
            name="hyena_back",
        )(*operands)
    )
    return tuple(
        pl.pallas_call(
            store_kernel,
            out_shape=[jax.ShapeDtypeStruct(r.shape, r.dtype) for r in results[:3]]
            + [jax.ShapeDtypeStruct((BLOCK, HALF), F32)],
            in_specs=[vmem] * 4,
            out_specs=[anywhere] * 4,
            scratch_shapes=[
                pltpu.VMEM((BLOCK, HALF), F32),
                pltpu.SemaphoreType.DMA((7,)),
            ],
            compiler_params=pltpu.CompilerParams(vmem_limit_bytes=4 * 1024 * 1024),
            name="store",
        )(*results)
    )


def solution(mesh):
    in_specs = (
        P("ch", "seq", None),
        P("ch", "seq", None),
        P("ch", "seq", None),
        P("ch", "seq", None),
        P("seq", None),
        P(),
    )
    out_specs = (P("ch", "seq", None), P("ch", "seq", None), P("ch", "seq", None), P("seq", "ch"))
    return jax.shard_map(shards, mesh=mesh, in_specs=in_specs, out_specs=out_specs, check_vma=False)
```
